32 devices in a mesh: dp: 1 (over z), tp: 32 (over y, x, core).
Axes of the slice: x: 4, y: 4, z: 1, core: 2. Of those that a mesh axis runs over, the one named last changes fastest.
The devices are a block of a 4x4x8 slice.
Arguments:
- hidden_in: bfloat16 [3, 1024, 4096], P('dp', 'tp')
- norms: float32 [2, 4, 4096], replicated
- w_qkv: bfloat16 [2, 4096, 3, 32, 128], P(None, None, None, 'tp')
- w_out: bfloat16 [2, 32, 128, 4096], P(None, 'tp')
- b_out: float32 [2, 4096], replicated
- w_up: bfloat16 [2, 4096, 16384], P(None, None, 'tp')
- b_up: float32 [2, 16384], P(None, 'tp')
- w_down: bfloat16 [2, 16384, 4096], P(None, 'tp')
- b_down: float32 [2, 4096], replicated
Outputs:
- output: bfloat16 [3, 1024, 4096], P('dp', 'tp')
All inputs are finite; a program needn't handle non-finite values.
Results may differ from the reference program's by a relative error of at most 0.0104407.
Values are sent between devices in bfloat16 or wider.
A program may use at most 768 MiB of HBM per device.

```python
import math
import jax
import jax.numpy as jnp
from jax import lax

N_BATCH = 3
SEQ_LEN = 1024
N_HEADS = 32
HEAD_DIM = 128
FF_DIM = 16384
N_LAYERS = 2

MODEL_DIM = N_HEADS * HEAD_DIM
LN_EPS = 1e-5


def setup_inputs(seed: int = 0, part: int = 0) -> dict:
    base_key = jax.random.key(seed)
    keys = jax.random.split(base_key, 9)
    part_key = jax.random.fold_in(keys[0], part)
    tok_key, scale_key = jax.random.split(part_key)
    tok_scale = jnp.exp(0.4 * jax.random.normal(scale_key, (N_BATCH, SEQ_LEN, 1), jnp.float32))
    hidden_in = (jax.random.normal(tok_key, (N_BATCH, SEQ_LEN, MODEL_DIM), jnp.float32) * tok_scale).astype(jnp.bfloat16)
    norm_base = jnp.array([1.0, 0.0, 1.0, 0.0], jnp.float32)[None, :, None]
    norms = norm_base + 0.2 * jax.random.normal(keys[1], (N_LAYERS, 4, MODEL_DIM), jnp.float32)
    qk_gain = (math.log(SEQ_LEN) / 2.0) ** 0.25
    slot_gain = jnp.array([qk_gain, qk_gain, 1.0], jnp.float32)[None, None, :, None, None]
    w_qkv = (jax.random.normal(keys[2], (N_LAYERS, MODEL_DIM, 3, N_HEADS, HEAD_DIM), jnp.float32) * slot_gain * MODEL_DIM ** -0.5).astype(jnp.bfloat16)
    out_gain = 0.7 * SEQ_LEN ** 0.25 * MODEL_DIM ** -0.5
    w_out = (jax.random.normal(keys[3], (N_LAYERS, N_HEADS, HEAD_DIM, MODEL_DIM), jnp.float32) * out_gain).astype(jnp.bfloat16)
    b_out = 0.2 * jax.random.normal(keys[4], (N_LAYERS, MODEL_DIM), jnp.float32)
    w_up = (jax.random.normal(keys[5], (N_LAYERS, MODEL_DIM, FF_DIM), jnp.float32) * MODEL_DIM ** -0.5).astype(jnp.bfloat16)
    b_up = 0.3 * jax.random.normal(keys[6], (N_LAYERS, FF_DIM), jnp.float32)
    w_down = (jax.random.normal(keys[7], (N_LAYERS, FF_DIM, MODEL_DIM), jnp.float32) * FF_DIM ** -0.5).astype(jnp.bfloat16)
    b_down = 0.2 * jax.random.normal(keys[8], (N_LAYERS, MODEL_DIM), jnp.float32)
    return {'hidden_in': hidden_in, 'norms': norms, 'w_qkv': w_qkv, 'w_out': w_out, 'b_out': b_out, 'w_up': w_up, 'b_up': b_up, 'w_down': w_down, 'b_down': b_down}


def layer_norm(rows, gain, shift):
    row_mean = jnp.mean(rows, axis=-1, keepdims=True)
    centred = rows - row_mean
    row_var = jnp.mean(centred * centred, axis=-1, keepdims=True)
    return (centred * lax.rsqrt(row_var + LN_EPS) * gain + shift).astype(jnp.bfloat16)


def one_head(head_qkv):
    queries = head_qkv[:, 0].astype(jnp.float32)
    keys_h = head_qkv[:, 1].astype(jnp.float32)
    values_h = head_qkv[:, 2].astype(jnp.float32)
    scores = jnp.einsum('bqe,bke->bqk', queries, keys_h) * HEAD_DIM ** -0.5
    attn_prob = jax.nn.softmax(scores, axis=-1).astype(jnp.bfloat16)
    return jnp.einsum('bqk,bke->bqe', attn_prob.astype(jnp.float32), values_h).astype(jnp.bfloat16)


def one_layer(residual, params):
    norm_l, wqkv_l, wout_l, bout_l, wup_l, bup_l, wdown_l, bdown_l = params
    normed = layer_norm(residual, norm_l[0], norm_l[1])
    qkv_heads = jnp.einsum('bsd,dthe->hbtse', normed.astype(jnp.float32), wqkv_l.astype(jnp.float32)).astype(jnp.bfloat16)
    attn_rows = lax.map(one_head, qkv_heads)
    attn_out = jnp.einsum('hbse,hed->bsd', attn_rows.astype(jnp.float32), wout_l.astype(jnp.float32))
    residual = residual + attn_out + bout_l
    normed2 = layer_norm(residual, norm_l[2], norm_l[3])
    hidden = jnp.einsum('bsd,df->bsf', normed2.astype(jnp.float32), wup_l.astype(jnp.float32)) + bup_l
    gelu_out = jax.nn.gelu(hidden, approximate=True).astype(jnp.bfloat16)
    mlp_out = jnp.einsum('bsf,fd->bsd', gelu_out.astype(jnp.float32), wdown_l.astype(jnp.float32))
    residual = residual + mlp_out + bdown_l
    return residual, None


def reference(hidden_in, norms, w_qkv, w_out, b_out, w_up, b_up, w_down, b_down):
    residual, unused = lax.scan(one_layer, hidden_in.astype(jnp.float32), (norms, w_qkv, w_out, b_out, w_up, b_up, w_down, b_down))
    return residual.astype(jnp.bfloat16)
```

```python
import functools
import math

import jax
import jax.numpy as jnp
from jax import lax
from jax.experimental import pallas as pl
from jax.experimental.pallas import tpu as pltpu
from jax.sharding import PartitionSpec as P

LN_EPS = 1e-5
MESH = pl.DeviceIdType.MESH
F32 = jnp.float32
BF16 = jnp.bfloat16
VMEM_LIMIT = 66_900_000
TILE = 16


class Place:
    def __init__(self, group_size):
        self.side = side = math.isqrt(group_size // 2)
        self.chips = side * side
        index = lax.axis_index("tp")
        self.core = index % 2
        chip = index // 2
        x, y = chip % side, chip // side
        self.first = x * (1 - self.core) + y * self.core
        self.second = y * (1 - self.core) + x * self.core
        self.pos = self.pos_of(self.first, self.second)

    def device(self, first, second):
        x = first * (1 - self.core) + second * self.core
        y = second * (1 - self.core) + first * self.core
        return {"tp": (y * self.side + x) * 2 + self.core}

    def partner(self):
        x = self.first * (1 - self.core) + self.second * self.core
        y = self.second * (1 - self.core) + self.first * self.core
        return {"tp": (y * self.side + x) * 2 + 1 - self.core}

    def pos_of(self, first, second):
        return second * self.side + (first + second) % self.side

    def at_pos(self, pos):
        second = pos // self.side
        return (pos % self.side + self.side - second) % self.side, second

    def barrier(self):
        barrier = pltpu.get_barrier_semaphore()
        peers = [self.device((self.first + d) % self.side, self.second) for d in range(1, self.side)]
        peers += [self.device(self.first, (self.second + d) % self.side) for d in range(1, self.side)]
        peers.append(self.partner())
        for peer in peers:
            pl.semaphore_signal(barrier, inc=1, device_id=peer, device_id_type=MESH)
        pl.semaphore_wait(barrier, len(peers))


def far_first(side):
    return sorted(range(1, side), key=lambda d: -min(d, side - d))


def remote(src, dst, send_sem, recv_sem, device):
    return pltpu.make_async_remote_copy(src_ref=src, dst_ref=dst, send_sem=send_sem, recv_sem=recv_sem, device_id=device, device_id_type=MESH)


def norm_rows(r_ref, gain, shift, buf):
    def rows_of(i, carry):
        rows = pl.ds(pl.multiple_of(i * TILE, TILE), TILE)
        v = r_ref[rows, :]
        mean = jnp.mean(v, axis=-1, keepdims=True)
        v = v - mean
        var = jnp.mean(v * v, axis=-1, keepdims=True)
        buf[0, rows, :] = (v * lax.rsqrt(var + LN_EPS) * gain + shift).astype(BF16)
        return carry
    lax.fori_loop(0, r_ref.shape[0] // TILE, rows_of, 0)


class Gather:
    def __init__(self, place, buf, send, recv):
        self.place, self.buf, self.send, self.recv = place, buf, send, recv
        self.half = buf.shape[1] // 2
        self.subs = self.half // TILE
        n = place.chips
        self.next = [place.device(*place.at_pos((place.pos + 1) % n)), place.device(*place.at_pos((place.pos + n - 1) % n))]

    def hop(self, dr, s, k):
        rows = pl.ds(dr * self.half + k * TILE, TILE)
        return remote(self.buf.at[s, rows], self.buf.at[s + 1, rows], self.send.at[dr, s, k], self.recv.at[dr, s, k], self.next[dr])

    def start(self):
        for k in range(self.subs):
            for dr in range(2):
                self.hop(dr, 0, k).start()

    def take(self, s, k):
        for dr in range(2):
            self.hop(dr, s - 1, k).wait_recv()

            @pl.when(s < self.place.chips - 1)
            def _():
                self.hop(dr, s, k).start()

    def sent(self, s):
        @pl.when(s < self.place.chips - 1)
        def _():
            for dr in range(2):
                for k in range(self.subs):
                    self.hop(dr, s, k).wait_send()

    def run(self, part):
        n = self.place.chips // 2
        for k in range(self.subs):
            self.take(1, k)

        def step(j, carry):
            for h in range(2):
                for k in range(self.subs):
                    self.take(2 * j + h, k)
                    part(j - 1, h * self.subs + k)
            return carry
        lax.fori_loop(1, n, step, 0)
        for i in range(2 * self.subs):
            part(n - 1, i)


class Scatter:
    def __init__(self, place, buf, r1, sums, r2, s1_send, s1_recv, s2_send, s2_recv):
        self.place, self.buf, self.r1, self.sums, self.r2 = place, buf, r1, sums, r2
        self.s1_send, self.s1_recv, self.s2_send, self.s2_recv = s1_send, s1_recv, s2_send, s2_recv
        self.half = buf.shape[1] // 2

    def rows(self, dr):
        return pl.ds(dr * self.half, self.half)

    def first_copy(self, slot, dr, j, first, second):
        p = self.place
        return remote(self.buf.at[slot, self.rows(dr)], self.r1.at[j, second, self.rows(dr)], self.s1_send.at[j, second, dr],
                      self.s1_recv.at[j, second, dr], p.device(first, p.second))

    def send_slot(self, slot):
        p = self.place
        for dr in range(2):
            pos = (p.pos + (p.chips - slot if dr == 0 else slot)) % p.chips
            first, second = p.at_pos(pos)
            away = (first + p.side - p.first) % p.side

            @pl.when(away != 0)
            def _():
                self.first_copy(slot, dr, p.side - 1 - away, first, second).start()

    def slot_of(self, first, second, dr):
        p = self.place
        pos = p.pos_of(first, second)
        return (p.pos + p.chips - pos) % p.chips if dr == 0 else (pos + p.chips - p.pos) % p.chips

    def send_owner(self, away, second, dr):
        p = self.place
        first = (p.first + away) % p.side
        self.first_copy(self.slot_of(first, second, dr), dr, p.side - 1 - away, first, second).start()

    def second_copy(self, d, dr):
        p = self.place
        return remote(self.sums.at[d - 1, self.rows(dr)], self.r2.at[p.side - 1 - d, self.rows(dr)], self.s2_send.at[p.side - 1 - d, dr],
                      self.s2_recv.at[p.side - 1 - d, dr], p.device(p.first, (p.second + d) % p.side))

    def finish(self, r_ref, bias_ref, out_ref):
        p = self.place
        peers = range(p.side - 1)

        def arrived(second, dr):
            for j in peers:
                self.first_copy(0, dr, j, p.first, second).wait_recv()

        def total(second, dr, rows):
            v = self.buf[self.slot_of(p.first, second, dr), rows, :].astype(F32)
            for j in peers:
                v = v + self.r1[j, second, rows, :].astype(F32)
            return v

        def each(dr, fn):
            def one(i, carry):
                fn(pl.ds(pl.multiple_of(dr * self.half + i * TILE, TILE), TILE))
                return carry
            lax.fori_loop(0, self.half // TILE, one, 0)

        for d in far_first(p.side):
            second = (p.second + d) % p.side
            for dr in range(2):
                arrived(second, dr)

                def store(rows):
                    self.sums[d - 1, rows, :] = total(second, dr, rows)
                each(dr, store)
                self.second_copy(d, dr).start()
        for dr in range(2):
            arrived(p.second, dr)
            for d in range(1, p.side):
                self.second_copy(d, dr).wait_recv()

            def last(rows):
                v = total(p.second, dr, rows)
                for j in peers:
                    v = v + self.r2[j, rows, :]
                out_ref[rows, :] = (r_ref[rows, :] + v + bias_ref[...]).astype(out_ref.dtype)
            each(dr, last)
        for dr in range(2):
            for j in peers:
                for second in range(p.side):
                    self.first_copy(0, dr, j, p.first, second).wait_send()
            for d in range(1, p.side):
                self.second_copy(d, dr).wait_send()


class Share:
    def __init__(self, place, pairs, local, send, recv):
        self.place, self.pairs, self.local, self.send, self.recv = place, pairs, local, send, recv

    def load(self, i):
        src, own, _ = self.pairs[i]
        return pltpu.make_async_copy(src, own, self.local.at[i])

    def give(self, i):
        _, own, other = self.pairs[i]
        return remote(own, other, self.send.at[i], self.recv.at[i], self.place.partner())


def attn_kernel(group_size, layer, head_dim, n_seq, r_ref, norm_ref, bias_ref, wqkv_ref, wout_ref, out_ref,
                buf, w, wo, qkv, kvp, att, r1, sums, r2, wl, ws, wr, ag_send, ag_recv, kv_send, kv_recv, s1_send, s1_recv, s2_send, s2_recv):
    place = Place(group_size)
    hd = head_dim
    slots, block = buf.shape[0], buf.shape[1]
    per_seq = block // n_seq
    share = Share(place, [(wqkv_ref.at[layer], w.at[:, pl.ds(0, 3 * hd)], w.at[:, pl.ds(3 * hd, 3 * hd)]),
                          (wout_ref.at[layer], wo.at[pl.ds(0, hd)], wo.at[pl.ds(hd, hd)])], wl, ws, wr)
    for i in range(2):
        share.load(i).start()
    norm_rows(r_ref, norm_ref[0:1, :], norm_ref[1:2, :], buf)
    place.barrier()
    gather = Gather(place, buf, ag_send, ag_recv)
    gather.start()
    for i in range(2):
        share.load(i).wait()
        share.give(i).start()

    def kv_copy(j, h):
        pair = pl.ds(2 * j, 2)
        return remote(qkv.at[pair, :, pl.ds(3 * hd * h + hd, 2 * hd)], kvp.at[pair, :, pl.ds(2 * hd * (1 - h), 2 * hd)],
                      kv_send.at[j, h], kv_recv.at[j, h], place.partner())

    wide = 6 * hd // 3

    def part(j, i):
        if i % 2 == 0:
            if i == 0:
                @pl.when(j == 0)
                def _():
                    share.give(0).wait_recv()
            cols = pl.ds(i // 2 * wide, wide)
            rows = buf[pl.ds(2 * j, 2)].reshape(2 * block, buf.shape[2])
            qkv[pl.ds(2 * j, 2), :, cols] = jnp.dot(rows, w[:, cols], preferred_element_type=F32).astype(BF16).reshape(2, block, wide)
        if i == 5:
            for h in range(2):
                kv_copy(j, h).start()
            gather.sent(2 * j)
            gather.sent(2 * j + 1)
    gather.run(part)
    for j in range(slots // 2):
        for h in range(2):
            kv_copy(j, h).wait_recv()

    q_slots = slots // 2
    nq, nk = q_slots * per_seq, slots * per_seq

    def head_of(i, carry):
        seq, h, qi = i // 4, i // 2 % 2, i % 2
        rows = pl.ds(pl.multiple_of(seq * per_seq, per_seq), per_seq)
        at = pl.ds(pl.multiple_of(qi * q_slots, q_slots), q_slots)

        def cols(base, width, k):
            return pl.ds(pl.multiple_of(h * width + k * hd, hd), hd)
        q = qkv[at, rows, cols(0, 3 * hd, 0)].reshape(nq, hd)
        k0 = qkv[:, rows, cols(0, 3 * hd, 1)].reshape(nk, hd)
        v0 = qkv[:, rows, cols(0, 3 * hd, 2)].reshape(nk, hd)
        k1 = kvp[:, rows, cols(0, 2 * hd, 0)].reshape(nk, hd)
        v1 = kvp[:, rows, cols(0, 2 * hd, 1)].reshape(nk, hd)
        dims = (((1,), (1,)), ((), ()))
        s0 = lax.dot_general(q, k0, dims, preferred_element_type=F32) * hd ** -0.5
        s1 = lax.dot_general(q, k1, dims, preferred_element_type=F32) * hd ** -0.5
        top = jnp.maximum(jnp.max(s0, axis=-1, keepdims=True), jnp.max(s1, axis=-1, keepdims=True))
        e0 = jnp.exp(s0 - top)
        e1 = jnp.exp(s1 - top)
        inv = 1.0 / (jnp.sum(e0, axis=-1, keepdims=True) + jnp.sum(e1, axis=-1, keepdims=True))
        a = jnp.dot((e0 * inv).astype(BF16), v0, preferred_element_type=F32)
        a = a + jnp.dot((e1 * inv).astype(BF16), v1, preferred_element_type=F32)
        att[at, rows, pl.ds(pl.multiple_of(h * hd, hd), hd)] = a.astype(BF16).reshape(q_slots, per_seq, hd)
        return carry
    lax.fori_loop(0, n_seq * 4, head_of, 0)

    share.give(1).wait_recv()
    scatter = Scatter(place, buf, r1, sums, r2, s1_send, s1_recv, s2_send, s2_recv)
    width = buf.shape[2] // 4

    def project(i, carry):
        j, c = i // 4, i % 4
        rows = att[pl.ds(2 * j, 2)].reshape(2 * block, 2 * hd)
        cols = pl.ds(pl.multiple_of(c * width, width), width)
        buf[pl.ds(2 * j, 2), :, cols] = jnp.dot(rows, wo[:, cols], preferred_element_type=F32).astype(BF16).reshape(2, block, width)
        return carry
    lax.fori_loop(0, slots * 2, project, 0)
    for d in (*far_first(place.side), 0):
        for away in far_first(place.side):
            for dr in range(2):
                scatter.send_owner(away, (place.second + d) % place.side, dr)
    scatter.finish(r_ref, bias_ref, out_ref)
    for i in range(2):
        share.give(i).wait_send()
    for j in range(slots // 2):
        for h in range(2):
            kv_copy(j, h).wait_send()


def mlp_kernel(group_size, layer, r_ref, norm_ref, bias_ref, bup_ref, wup_ref, wdown_ref, out_ref,
               buf, wu, wd, bu, u, r1, sums, r2, wl, ws, wr, ag_send, ag_recv, s1_send, s1_recv, s2_send, s2_recv):
    place = Place(group_size)
    slots, block, model = buf.shape
    ff = wup_ref.shape[2]
    share = Share(place, [(bup_ref.at[pl.ds(layer, 1)], bu.at[:, pl.ds(0, ff)], bu.at[:, pl.ds(ff, ff)]),
                          (wup_ref.at[layer], wu.at[:, pl.ds(0, ff)], wu.at[:, pl.ds(ff, ff)]),
                          (wdown_ref.at[layer], wd.at[pl.ds(0, ff)], wd.at[pl.ds(ff, ff)])], wl, ws, wr)
    for i in range(3):
        share.load(i).start()
    norm_rows(r_ref, norm_ref[2:3, :], norm_ref[3:4, :], buf)
    place.barrier()
    gather = Gather(place, buf, ag_send, ag_recv)
    gather.start()
    for i in range(3):
        share.load(i).wait()
        share.give(i).start()
    scatter = Scatter(place, buf, r1, sums, r2, s1_send, s1_recv, s2_send, s2_recv)
    up_w, down_w = ff // 2, model // 4

    def up(j, c):
        rows = buf[pl.ds(2 * j, 2)].reshape(2 * block, model)
        cols = pl.ds(c * up_w, up_w)
        hidden = jnp.dot(rows, wu[:, cols], preferred_element_type=F32) + bu[:, cols]
        u[:, cols] = jax.nn.gelu(hidden, approximate=True).astype(BF16)

    def down(j, c):
        cols = pl.ds(c * down_w, down_w)
        buf[pl.ds(2 * j, 2), :, cols] = jnp.dot(u[...], wd[:, cols], preferred_element_type=F32).astype(BF16).reshape(2, block, down_w)

    def part(j, i):
        if i == 0:
            @pl.when(j == 0)
            def _():
                share.give(0).wait_recv()
                share.give(1).wait_recv()
            up(j, 0)
            up(j, 1)
        elif i == 1:
            up(j, 2)
        elif i == 2:
            up(j, 3)
        elif i == 3:
            @pl.when(j == 0)
            def _():
                share.give(2).wait_recv()
            gather.sent(2 * j)
            gather.sent(2 * j + 1)
            down(j, 0)
        elif i == 4:
            down(j, 1)
        else:
            down(j, 2)
            down(j, 3)
            scatter.send_slot(2 * j)
            scatter.send_slot(2 * j + 1)
    gather.run(part)
    scatter.finish(r_ref, bias_ref, out_ref)
    for i in range(3):
        share.give(i).wait_send()


def solution(mesh):
    group_size = mesh.shape["tp"]
    side = math.isqrt(group_size // 2)
    chips = side * side
    dma = pltpu.SemaphoreType.DMA
    vmem = pl.BlockSpec(memory_space=pltpu.VMEM)
    hbm = pl.BlockSpec(memory_space=pl.ANY)

    def local_layers(hidden_in, norms, w_qkv, w_out, b_out, w_up, b_up, w_down, b_down):
        n_seq, per_seq, model = hidden_in.shape
        n_layers, head_dim, ff = w_qkv.shape[0], w_qkv.shape[-1], w_up.shape[-1]
        block = n_seq * per_seq
        subs = block // 2 // TILE
        residual = hidden_in.astype(F32).reshape(block, model)
        w_qkv = w_qkv.reshape(n_layers, model, 3 * head_dim)
        w_out = w_out.reshape(n_layers, head_dim, model)
        ring = [dma((2, chips - 1, subs))] * 2
        reduce_bufs = [pltpu.VMEM((side - 1, side, block, model), BF16), pltpu.VMEM((side - 1, block, model), F32),
                       pltpu.VMEM((side - 1, block, model), F32)]
        reduce_sems = [dma((side - 1, side, 2))] * 2 + [dma((side - 1, 2))] * 2
        rows = pltpu.VMEM((chips, block, model), BF16)

        def params(collective_id):
            return pltpu.CompilerParams(collective_id=collective_id, has_side_effects=True, vmem_limit_bytes=VMEM_LIMIT)

        for layer in range(n_layers):
            residual = pl.pallas_call(
                functools.partial(attn_kernel, group_size, layer, head_dim, n_seq), name=f"attn{layer}",
                out_shape=jax.ShapeDtypeStruct((block, model), F32),
                in_specs=[vmem, vmem, vmem, hbm, hbm], out_specs=vmem,
                scratch_shapes=[rows, pltpu.VMEM((model, 6 * head_dim), BF16), pltpu.VMEM((2 * head_dim, model), BF16),
                                pltpu.VMEM((chips, block, 6 * head_dim), BF16), pltpu.VMEM((chips, block, 4 * head_dim), BF16),
                                pltpu.VMEM((chips, block, 2 * head_dim), BF16), *reduce_bufs, dma((2,)), dma((2,)), dma((2,)), *ring,
                                dma((chips // 2, 2)), dma((chips // 2, 2)), *reduce_sems],
                compiler_params=params(2 * layer),
            )(residual, norms[layer], b_out[layer][None], w_qkv, w_out)
            residual = pl.pallas_call(
                functools.partial(mlp_kernel, group_size, layer), name=f"mlp{layer}",
                out_shape=jax.ShapeDtypeStruct((block, model), F32 if layer < n_layers - 1 else BF16),
                in_specs=[vmem, vmem, vmem, hbm, hbm, hbm], out_specs=vmem,
                scratch_shapes=[rows, pltpu.VMEM((model, 2 * ff), BF16), pltpu.VMEM((2 * ff, model), BF16), pltpu.VMEM((1, 2 * ff), F32),
                                pltpu.VMEM((2 * block, 2 * ff), BF16), *reduce_bufs, dma((3,)), dma((3,)), dma((3,)), *ring, *reduce_sems],
                compiler_params=params(2 * layer + 1),
            )(residual, norms[layer], b_down[layer][None], b_up, w_up, w_down)
        return residual.reshape(n_seq, per_seq, model)

    in_specs = (P('dp', 'tp', None), P(), P(None, None, None, 'tp', None), P(None, 'tp', None, None), P(), P(None, None, 'tp'), P(None, 'tp'), P(None, 'tp', None), P())
    return jax.shard_map(local_layers, mesh=mesh, in_specs=in_specs, out_specs=P('dp', 'tp', None), check_vma=False)
```

```python
import functools
import math

import jax
import jax.numpy as jnp
from jax import lax
from jax.experimental import pallas as pl
from jax.experimental.pallas import tpu as pltpu
from jax.sharding import PartitionSpec as P

LN_EPS = 1e-5
MESH = pl.DeviceIdType.MESH
F32 = jnp.float32
BF16 = jnp.bfloat16
VMEM_LIMIT = 66_900_000
TILE = 16


class Place:
    def __init__(self, group_size):
        self.side = side = math.isqrt(group_size // 2)
        self.chips = side * side
        index = lax.axis_index("tp")
        self.core = index % 2
        chip = index // 2
        x, y = chip % side, chip // side
        self.first = x * (1 - self.core) + y * self.core
        self.second = y * (1 - self.core) + x * self.core
        self.pos = self.pos_of(self.first, self.second)

    def device(self, first, second):
        x = first * (1 - self.core) + second * self.core
        y = second * (1 - self.core) + first * self.core
        return {"tp": (y * self.side + x) * 2 + self.core}

    def partner(self):
        x = self.first * (1 - self.core) + self.second * self.core
        y = self.second * (1 - self.core) + self.first * self.core
        return {"tp": (y * self.side + x) * 2 + 1 - self.core}

    def pos_of(self, first, second):
        return second * self.side + (first + second) % self.side

    def at_pos(self, pos):
        second = pos // self.side
        return (pos % self.side + self.side - second) % self.side, second

    def peers(self):
        peers = [self.device((self.first + d) % self.side, self.second) for d in range(1, self.side)]
        peers += [self.device(self.first, (self.second + d) % self.side) for d in range(1, self.side)]
        return [*peers, self.partner()]

    def greet(self):
        for peer in self.peers():
            pl.semaphore_signal(pltpu.get_barrier_semaphore(), inc=1, device_id=peer, device_id_type=MESH)

    def meet(self):
        pl.semaphore_wait(pltpu.get_barrier_semaphore(), 2 * self.side - 1)


def far_first(side):
    return sorted(range(1, side), key=lambda d: -min(d, side - d))


def remote(src, dst, send_sem, recv_sem, device):
    return pltpu.make_async_remote_copy(src_ref=src, dst_ref=dst, send_sem=send_sem, recv_sem=recv_sem, device_id=device, device_id_type=MESH)


def norm_rows(r_ref, gain, shift, buf, tile):
    rows = pl.ds(pl.multiple_of(tile * TILE, TILE), TILE)
    v = r_ref[rows, :].astype(F32)
    mean = jnp.mean(v, axis=-1, keepdims=True)
    v = v - mean
    var = jnp.mean(v * v, axis=-1, keepdims=True)
    buf[0, rows, :] = (v * lax.rsqrt(var + LN_EPS) * gain + shift).astype(BF16)


class Gather:
    def __init__(self, place, buf, send, recv):
        self.place, self.buf, self.send, self.recv = place, buf, send, recv
        self.half = buf.shape[1] // 2
        self.subs = self.half // TILE
        n = place.chips
        self.next = [place.device(*place.at_pos((place.pos + 1) % n)), place.device(*place.at_pos((place.pos + n - 1) % n))]

    def hop(self, dr, s, k):
        rows = pl.ds(dr * self.half + k * TILE, TILE)
        return remote(self.buf.at[s, rows], self.buf.at[s + 1, rows], self.send.at[dr, s, k], self.recv.at[dr, s, k], self.next[dr])

    def start(self, norm, before, meanwhile):
        norm(0)
        norm(self.subs)
        self.place.meet()
        before()

        def step(k, carry):
            norm(k)
            norm(self.subs + k)
            for dr in range(2):
                self.hop(dr, 0, k - 1).start()
            return carry
        lax.fori_loop(1, self.subs, step, 0)
        meanwhile()
        for dr in range(2):
            self.hop(dr, 0, self.subs - 1).start()

    def take(self, s, k):
        for dr in range(2):
            self.hop(dr, s - 1, k).wait_recv()

            @pl.when(s < self.place.chips - 1)
            def _():
                self.hop(dr, s, k).start()

    def sent(self, s):
        @pl.when(s < self.place.chips - 1)
        def _():
            for dr in range(2):
                for k in range(self.subs):
                    self.hop(dr, s, k).wait_send()

    def run(self, part):
        n = self.place.chips // 2
        for k in range(self.subs):
            self.take(1, k)

        def step(j, carry):
            for h in range(2):
                for k in range(self.subs):
                    @pl.when(j < n)
                    def _():
                        self.take(2 * j + h, k)
                    part(j - 1, h * self.subs + k)
            return carry
        lax.fori_loop(1, n + 1, step, 0)


class Scatter:
    def __init__(self, place, buf, r1, sums, mid, r2, s1_send, s1_recv, mid_send, mid_recv, s2_send, s2_recv):
        self.place, self.buf, self.r1, self.sums, self.mid, self.r2 = place, buf, r1, sums, mid, r2
        self.mid_send, self.mid_recv = mid_send, mid_recv
        self.s1_send, self.s1_recv, self.s2_send, self.s2_recv = s1_send, s1_recv, s2_send, s2_recv
        self.half = buf.shape[1] // 2

    def rows(self, dr):
        return pl.ds(dr * self.half, self.half)

    def first_copy(self, slot, dr, j, first, second):
        p = self.place
        return remote(self.buf.at[slot, self.rows(dr)], self.r1.at[j, second, self.rows(dr)], self.s1_send.at[j, second, dr],
                      self.s1_recv.at[j, second, dr], p.device(first, p.second))

    def send_slot(self, slot):
        p = self.place
        for dr in range(2):
            pos = (p.pos + (p.chips - slot if dr == 0 else slot)) % p.chips
            first, second = p.at_pos(pos)
            away = (first + p.side - p.first) % p.side

            @pl.when(away != 0)
            def _():
                self.first_copy(slot, dr, p.side - 1 - away, first, second).start()

    def slot_of(self, first, second, dr):
        p = self.place
        pos = p.pos_of(first, second)
        return (p.pos + p.chips - pos) % p.chips if dr == 0 else (pos + p.chips - p.pos) % p.chips

    def arrived(self, second, dr):
        for j in range(self.place.side - 1):
            self.first_copy(0, dr, j, self.place.first, second).wait_recv()

    def total(self, second, dr, rows):
        v = self.buf[self.slot_of(self.place.first, second, dr), rows, :].astype(F32)
        for j in range(self.place.side - 1):
            v = v + self.r1[j, second, rows, :].astype(F32)
        return v

    def tile(self, dr, k):
        return pl.ds(pl.multiple_of(dr * self.half + k * TILE, TILE), TILE)

    def mid_copy(self, dr, k):
        p = self.place
        step = 1 if dr == 0 else p.side - 1
        rows = self.tile(dr, k)
        return remote(self.sums.at[1, rows], self.mid.at[rows], self.mid_send.at[dr, k], self.mid_recv.at[dr, k],
                      p.device(p.first, (p.second + step) % p.side))

    def end_copy(self, d, dr, k):
        p = self.place
        at = 0 if d == 1 else 1
        rows = self.tile(dr, k)
        return remote(self.sums.at[d - 1, rows], self.r2.at[at, rows], self.s2_send.at[at, dr, k], self.s2_recv.at[at, dr, k],
                      p.device(p.first, (p.second + d) % p.side))

    def add(self, d, dr, k, with_mid):
        second = (self.place.second + d) % self.place.side
        rows = self.tile(dr, k)
        v = self.total(second, dr, rows)
        if with_mid:
            self.mid_copy(dr, k).wait_recv()
            v = v + self.mid[rows, :]
        self.sums[d - 1, rows, :] = v

    def tiles(self, fn):
        def one(k, carry):
            fn(k)
            return carry
        lax.fori_loop(0, self.half // TILE, one, 0)

    def finish(self, r_ref, bias, out_ref):
        p = self.place

        def pieces(group, with_mid, copy):
            for d, dr in group:
                self.arrived((p.second + d) % p.side, dr)

            def one(k):
                for d, dr in group:
                    self.add(d, dr, k, with_mid)
                    copy(d, dr, k).start()
            self.tiles(one)

        ends = [(1, 1), (p.side - 1, 0)] if p.side > 2 else [(1, 0), (1, 1)]
        pieces(ends, False, self.end_copy)
        if p.side > 2:
            pieces([(2, 0), (2, 1)], False, lambda d, dr, k: self.mid_copy(dr, k))
            more = [(1, 0), (p.side - 1, 1)]
            pieces(more, True, self.end_copy)
            ends = ends + more
        for dr in range(2):
            self.arrived(p.second, dr)

        def last(k):
            for dr in range(2):
                rows = self.tile(dr, k)
                for d, half in ends:
                    if half == dr:
                        self.end_copy(d, dr, k).wait_recv()
                v = self.total(p.second, dr, rows)
                for j in range(self.r2.shape[0]):
                    v = v + self.r2[j, rows, :]
                out_ref[rows, :] = (r_ref[rows, :] + v + bias).astype(out_ref.dtype)
        self.tiles(last)

        def sent(k):
            if p.side > 2:
                for dr in range(2):
                    self.mid_copy(dr, k).wait_send()
            for d, dr in ends:
                self.end_copy(d, dr, k).wait_send()
        self.tiles(sent)
        for dr in range(2):
            for j in range(p.side - 1):
                for second in range(p.side):
                    self.first_copy(0, dr, j, p.first, second).wait_send()


class Share:
    def __init__(self, place, pairs, local, send, recv):
        self.place, self.pairs, self.local, self.send, self.recv = place, pairs, local, send, recv

    def load(self, i):
        src, own, _ = self.pairs[i]
        return pltpu.make_async_copy(src, own, self.local.at[i])

    def give(self, i):
        _, own, other = self.pairs[i]
        return remote(own, other, self.send.at[i], self.recv.at[i], self.place.partner())


def attn_kernel(group_size, layer, n_seq, r_ref, norm_ref, bias_ref, wqkv_ref, wout_ref, out_ref,
                buf, w, wo, qkv, kvp, att, atts, w4, psum, r1, sums, r2, wl, ws, wr, ag_send, ag_recv, kv_send, kv_recv,
                at_send, at_recv, f_send, f_recv, w4_send, w4_recv, s1_send, s1_recv, s2_send, s2_recv):
    place = Place(group_size)
    side, n_chunks, hd = place.side, att.shape[0], att.shape[3] // 2
    slots, block, model = buf.shape
    per_seq = block // n_seq
    per_chunk = block // n_chunks
    width = model // side
    share = Share(place, [(wout_ref.at[layer], wo.at[pl.ds(0, hd)], wo.at[pl.ds(hd, hd)])]
                  + [(wqkv_ref.at[layer, t], w.at[:, pl.ds(t * hd, hd)], w.at[:, pl.ds((3 + t) * hd, hd)]) for t in range(3)], wl, ws, wr)
    place.greet()
    for i in range(4):
        share.load(i).start()
    gather = Gather(place, buf, ag_send, ag_recv)

    def norm(tile):
        norm_rows(r_ref, norm_ref[layer, 0:1, :], norm_ref[layer, 1:2, :], buf, tile)

    def col(first):
        return pl.ds(pl.multiple_of(first * width, width), width)

    def w_copy(d, h):
        first = (place.first + d) % side
        rows = pl.ds(h * hd, hd)
        return remote(wo.at[rows, col(first)], w4.at[side - 1 - d, rows], w4_send.at[side - 1 - d, h], w4_recv.at[side - 1 - d, h],
                      place.device(first, place.second))

    def share_out():
        share.load(0).wait()
        share.give(0).start()
        for d in far_first(side):
            w_copy(d, 0).start()

    def share_qkv():
        for i in range(1, 4):
            share.load(i).wait()
            share.give(i).start()
    gather.start(norm, share_out, share_qkv)
    share.give(0).wait_recv()
    for d in far_first(side):
        w_copy(d, 1).start()

    def kv_copy(j, h):
        pair = pl.ds(2 * j, 2)
        return remote(qkv.at[pair, :, pl.ds(3 * hd * h + hd, 2 * hd)], kvp.at[pair, :, pl.ds(2 * hd * (1 - h), 2 * hd)],
                      kv_send.at[j, h], kv_recv.at[j, h], place.partner())

    wide = 2 * hd

    def part(j, i):
        if i % 2 == 0:
            if i == 0:
                @pl.when(j == 0)
                def _():
                    for t in range(3):
                        share.give(1 + t).wait_recv()
            cols = pl.ds(i // 2 * wide, wide)
            rows = buf[pl.ds(2 * j, 2)].reshape(2 * block, model)
            qkv[pl.ds(2 * j, 2), :, cols] = jnp.dot(rows, w[:, cols], preferred_element_type=F32).astype(BF16).reshape(2, block, wide)
        if i == 5:
            for h in range(2):
                kv_copy(j, h).start()
            gather.sent(2 * j)
            gather.sent(2 * j + 1)
    gather.run(part)

    for j in range(slots // 2):
        for h in range(2):
            kv_copy(j, h).wait_recv()

    nq, nk = slots * per_chunk, slots * per_seq

    def rows_of(chunk):
        return pl.ds(pl.multiple_of(chunk * per_chunk, per_chunk), per_chunk)

    def attend(chunk):
        seq = chunk * per_chunk // per_seq
        lower = chunk * per_chunk // (block // 2)
        keys = pl.ds(pl.multiple_of(seq * per_seq, per_seq), per_seq)

        def head_of(h, carry):
            def cols(base, k):
                return pl.ds(pl.multiple_of(h * base + k * hd, hd), hd)
            q = qkv[:, rows_of(chunk), cols(3 * hd, 0)].reshape(nq, hd)
            k0 = qkv[:, keys, cols(3 * hd, 1)].reshape(nk, hd)
            v0 = qkv[:, keys, cols(3 * hd, 2)].reshape(nk, hd)
            k1 = kvp[:, keys, cols(2 * hd, 0)].reshape(nk, hd)
            v1 = kvp[:, keys, cols(2 * hd, 1)].reshape(nk, hd)
            dims = (((1,), (1,)), ((), ()))
            s0 = lax.dot_general(q, k0, dims, preferred_element_type=F32) * hd ** -0.5
            s1 = lax.dot_general(q, k1, dims, preferred_element_type=F32) * hd ** -0.5
            top = jnp.maximum(jnp.max(s0, axis=-1, keepdims=True), jnp.max(s1, axis=-1, keepdims=True))
            e0 = jnp.exp(s0 - top)
            e1 = jnp.exp(s1 - top)
            inv = 1.0 / (jnp.sum(e0, axis=-1, keepdims=True) + jnp.sum(e1, axis=-1, keepdims=True))
            a = jnp.dot((e0 * inv).astype(BF16), v0, preferred_element_type=F32)
            a = (a + jnp.dot((e1 * inv).astype(BF16), v1, preferred_element_type=F32)).astype(BF16)
            for slot in range(slots):
                pos = (place.pos + (slots - slot) * (1 - lower) + slot * lower) % slots
                att[chunk, pos, :, cols(hd, 0)] = a[slot * per_chunk:(slot + 1) * per_chunk]
            return carry
        lax.fori_loop(0, 2, head_of, 0)
        for d in near:
            a_copy(chunk, d).start()

    near = [d for d in range(1, side) if min(d, side - d) == 1]

    def f_copy(seq, h):
        cols = pl.ds(h * hd, hd)
        return remote(atts.at[side - 2 if h == 0 else 0, seq, :, :, cols], atts.at[1, seq, :, :, cols], f_send.at[seq, h], f_recv.at[seq, h],
                      place.device((place.first + (1 if h == 0 else side - 1)) % side, place.second))

    def forward(seq):
        for d in near:
            a_copy(seq, d).wait_recv()
        if side > 2:
            for h in range(2):
                f_copy(seq, h).start()

    def a_copy(seq, d):
        return remote(att.at[seq], atts.at[side - 1 - d, seq], at_send.at[seq, side - 1 - d], at_recv.at[seq, side - 1 - d],
                      place.device((place.first + d) % side, place.second))

    def p_copy(seq, d):
        second = (place.second + d) % side
        return remote(psum.at[seq, pl.ds(pl.multiple_of(second * side, side), side)], r1.at[side - 1 - d, seq], s1_send.at[seq, side - 1 - d],
                      s1_recv.at[seq, side - 1 - d], place.device(place.first, second))

    def project(seq):
        @pl.when(seq == 0)
        def _():
            for d in range(1, side):
                for h in range(2):
                    w_copy(d, h).wait_recv()
        if side > 2:
            for h in range(2):
                f_copy(seq, h).wait_recv()
        half = width // 2
        for c in range(2):
            own = pl.ds(pl.multiple_of(place.first * width + c * half, half), half)
            cols = pl.ds(c * half, half)
            v = jnp.dot(att[seq].reshape(slots * per_chunk, 2 * hd), wo[:, own], preferred_element_type=F32)
            for j in range(side - 1):
                v = v + jnp.dot(atts[j, seq].reshape(slots * per_chunk, 2 * hd), w4[j, :, cols], preferred_element_type=F32)
            psum[seq, :, :, cols] = v.astype(BF16).reshape(slots, per_chunk, half)
        for d in far_first(side):
            p_copy(seq, d).start()

    def s_copy(seq, d):
        first = (place.first + d) % side
        return remote(sums.at[seq, (first + place.second) % side], r2.at[side - 1 - d, seq], s2_send.at[seq, side - 1 - d],
                      s2_recv.at[seq, side - 1 - d], place.device(first, place.second))

    def add(seq):
        for d in range(1, side):
            p_copy(seq, d).wait_recv()

        def one(i, carry):
            v = psum[seq, place.second * side + i].astype(F32)
            for j in range(side - 1):
                v = v + r1[j, seq, i].astype(F32)
            sums[seq, i] = v
            return carry
        lax.fori_loop(0, side, one, 0)
        for d in far_first(side):
            s_copy(seq, d).start()

    def output(seq):
        rows = rows_of(seq)

        def put(first, v):
            out_ref[rows, col(first)] = r_ref[rows, col(first)].astype(F32) + v + bias_ref[pl.ds(layer, 1), col(first)]
        put(place.first, sums[seq, (place.first + place.second) % side])
        for j in range(side - 1):
            s_copy(seq, side - 1 - j).wait_recv()
            put((place.first + 1 + j) % side, r2[j, seq])

    lag = n_chunks // 2
    stages = ((attend, 0), (forward, lag - 1), (project, lag), (add, lag + 1), (output, lag + 2))

    def step(i, carry):
        for stage, at in stages:
            @pl.when((i >= at) & (i < at + n_chunks))
            def _():
                stage(i - at)
        return carry
    lax.fori_loop(0, n_chunks + lag + 2, step, 0)
    for i in range(4):
        share.give(i).wait_send()
    for j in range(slots // 2):
        for h in range(2):
            kv_copy(j, h).wait_send()
    for d in range(1, side):
        for h in range(2):
            w_copy(d, h).wait_send()
        for seq in range(n_chunks):
            if d in near:
                a_copy(seq, d).wait_send()
            elif d == 2:
                for h in range(2):
                    f_copy(seq, h).wait_send()
            p_copy(seq, d).wait_send()
            s_copy(seq, d).wait_send()


def mlp_kernel(group_size, layer, r_ref, norm_ref, bias_ref, bup_ref, wup_ref, wdown_ref, out_ref,
               buf, wu, wd, bu, u, r1, sums, mid, r2, wl, ws, wr, ag_send, ag_recv, s1_send, s1_recv, mid_send, mid_recv, s2_send, s2_recv):
    place = Place(group_size)
    slots, block, model = buf.shape
    ff = wup_ref.shape[2]
    share = Share(place, [(bup_ref.at[pl.ds(layer, 1)], bu.at[:, pl.ds(0, ff)], bu.at[:, pl.ds(ff, ff)]),
                          (wup_ref.at[layer], wu.at[:, pl.ds(0, ff)], wu.at[:, pl.ds(ff, ff)]),
                          (wdown_ref.at[layer], wd.at[pl.ds(0, ff)], wd.at[pl.ds(ff, ff)])], wl, ws, wr)
    place.greet()
    for i in range(3):
        share.load(i).start()
    gather = Gather(place, buf, ag_send, ag_recv)

    def norm(tile):
        norm_rows(r_ref, norm_ref[layer, 2:3, :], norm_ref[layer, 3:4, :], buf, tile)

    def share_all():
        for i in range(3):
            share.load(i).wait()
            share.give(i).start()
    gather.start(norm, lambda: None, share_all)
    scatter = Scatter(place, buf, r1, sums, mid, r2, s1_send, s1_recv, mid_send, mid_recv, s2_send, s2_recv)
    up_w, down_w = ff // 2, model // 4
    def up(j, c):
        rows = buf[pl.ds(2 * j, 2)].reshape(2 * block, model)
        cols = pl.ds(c * up_w, up_w)
        hidden = jnp.dot(rows, wu[:, cols], preferred_element_type=F32) + bu[:, cols]
        u[:, cols] = jax.nn.gelu(hidden, approximate=True).astype(BF16)

    def down(j, c):
        cols = pl.ds(c * down_w, down_w)
        buf[pl.ds(2 * j, 2), :, cols] = jnp.dot(u[...], wd[:, cols], preferred_element_type=F32).astype(BF16).reshape(2, block, down_w)

    def send_slots(begin, end):
        def one(slot, carry):
            scatter.send_slot(slot)
            return carry
        lax.fori_loop(begin, end, one, 0)

    def part(j, i):
        if i == 0:
            @pl.when(j == 0)
            def _():
                share.give(0).wait_recv()
                share.give(1).wait_recv()

            @pl.when(j == slots // 2 - 1)
            def _():
                send_slots(0, slots - 2)
            up(j, 0)
            up(j, 1)
        elif i == 1:
            up(j, 2)
        elif i == 2:
            up(j, 3)
        elif i == 3:
            @pl.when(j == 0)
            def _():
                share.give(2).wait_recv()
            gather.sent(2 * j)
            gather.sent(2 * j + 1)
            down(j, 0)
        elif i == 4:
            down(j, 1)
        else:
            down(j, 2)
            down(j, 3)
    gather.run(part)
    send_slots(slots - 2, slots)
    scatter.finish(r_ref, bias_ref[pl.ds(layer, 1), :], out_ref)
    for i in range(3):
        share.give(i).wait_send()


def solution(mesh):
    group_size = mesh.shape["tp"]
    side = math.isqrt(group_size // 2)
    chips = side * side
    dma = pltpu.SemaphoreType.DMA
    vmem = pl.BlockSpec(memory_space=pltpu.VMEM)
    hbm = pl.BlockSpec(memory_space=pl.ANY)

    def local_layers(hidden_in, norms, w_qkv, w_out, b_out, w_up, b_up, w_down, b_down):
        n_seq, per_seq, model = hidden_in.shape
        n_layers, head_dim, ff = w_qkv.shape[0], w_qkv.shape[-1], w_up.shape[-1]
        block = n_seq * per_seq
        subs = block // 2 // TILE
        n_chunks = block // TILE
        residual = hidden_in.reshape(block, model)
        w_qkv = w_qkv.transpose(0, 2, 3, 1, 4).reshape(n_layers, 3, model, head_dim)
        w_out = w_out.reshape(n_layers, head_dim, model)
        width = model // side
        ring = [dma((2, chips - 1, subs))] * 2
        rows = pltpu.VMEM((chips, block, model), BF16)

        def params(collective_id):
            return pltpu.CompilerParams(collective_id=collective_id, has_side_effects=True, vmem_limit_bytes=VMEM_LIMIT)

        for layer in range(n_layers):
            residual = pl.pallas_call(
                functools.partial(attn_kernel, group_size, layer, n_seq), name=f"attn{layer}",
                out_shape=jax.ShapeDtypeStruct((block, model), F32),
                in_specs=[vmem, vmem, vmem, hbm, hbm], out_specs=vmem,
                scratch_shapes=[rows, pltpu.VMEM((model, 6 * head_dim), BF16), pltpu.VMEM((2 * head_dim, model), BF16),
                                pltpu.VMEM((chips, block, 6 * head_dim), BF16), pltpu.VMEM((chips, block, 4 * head_dim), BF16),
                                pltpu.VMEM((n_chunks, chips, TILE, 2 * head_dim), BF16),
                                pltpu.VMEM((side - 1, n_chunks, chips, TILE, 2 * head_dim), BF16),
                                pltpu.VMEM((side - 1, 2 * head_dim, width), BF16),
                                pltpu.VMEM((n_chunks, chips, TILE, width), BF16),
                                pltpu.VMEM((side - 1, n_chunks, side, TILE, width), BF16),
                                pltpu.VMEM((n_chunks, side, TILE, width), F32),
                                pltpu.VMEM((side - 1, n_chunks, TILE, width), F32),
                                dma((4,)), dma((4,)), dma((4,)), *ring, dma((chips // 2, 2)), dma((chips // 2, 2)),
                                *[dma((n_chunks, side - 1))] * 2, *[dma((n_chunks, 2))] * 2, *[dma((side - 1, 2))] * 2,
                                *[dma((n_chunks, side - 1))] * 4],
                compiler_params=params(2 * layer),
            )(residual, norms, b_out, w_qkv, w_out)
            residual = pl.pallas_call(
                functools.partial(mlp_kernel, group_size, layer), name=f"mlp{layer}",
                out_shape=jax.ShapeDtypeStruct((block, model), F32 if layer < n_layers - 1 else BF16),
                in_specs=[vmem, vmem, vmem, hbm, hbm, hbm], out_specs=vmem,
                scratch_shapes=[rows, pltpu.VMEM((model, 2 * ff), BF16), pltpu.VMEM((2 * ff, model), BF16), pltpu.VMEM((1, 2 * ff), F32),
                                pltpu.VMEM((2 * block, 2 * ff), BF16), pltpu.VMEM((side - 1, side, block, model), BF16),
                                pltpu.VMEM((side - 1, block, model), F32), pltpu.VMEM((block, model), F32),
                                pltpu.VMEM((min(2, side - 1), block, model), F32), dma((3,)), dma((3,)), dma((3,)), *ring,
                                *[dma((side - 1, side, 2))] * 2, *[dma((2, subs))] * 2, *[dma((2, 2, subs))] * 2],
                compiler_params=params(2 * layer + 1),
            )(residual, norms, b_down, b_up, w_up, w_down)
        return residual.reshape(n_seq, per_seq, model)

    in_specs = (P('dp', 'tp', None), P(), P(None, None, None, 'tp', None), P(None, 'tp', None, None), P(), P(None, None, 'tp'), P(None, 'tp'), P(None, 'tp', None), P())
    return jax.shard_map(local_layers, mesh=mesh, in_specs=in_specs, out_specs=P('dp', 'tp', None), check_vma=False)
```

```python
import functools
import math

import jax
import jax.numpy as jnp
from jax import lax
from jax.experimental import pallas as pl
from jax.experimental.pallas import tpu as pltpu
from jax.sharding import PartitionSpec as P

LN_EPS = 1e-5
MESH = pl.DeviceIdType.MESH
F32 = jnp.float32
BF16 = jnp.bfloat16
VMEM_LIMIT = 66_900_000
TILE = 16


class Place:
    def __init__(self, group_size):
        self.side = side = math.isqrt(group_size // 2)
        self.chips = side * side
        index = lax.axis_index("tp")
        self.core = index % 2
        chip = index // 2
        x, y = chip % side, chip // side
        self.first = x * (1 - self.core) + y * self.core
        self.second = y * (1 - self.core) + x * self.core
        self.pos = self.pos_of(self.first, self.second)

    def device(self, first, second):
        x = first * (1 - self.core) + second * self.core
        y = second * (1 - self.core) + first * self.core
        return {"tp": (y * self.side + x) * 2 + self.core}

    def partner(self):
        x = self.first * (1 - self.core) + self.second * self.core
        y = self.second * (1 - self.core) + self.first * self.core
        return {"tp": (y * self.side + x) * 2 + 1 - self.core}

    def pos_of(self, first, second):
        return second * self.side + (first + second) % self.side

    def at_pos(self, pos):
        second = pos // self.side
        return (pos % self.side + self.side - second) % self.side, second

    def peers(self):
        peers = [self.device((self.first + d) % self.side, self.second) for d in range(1, self.side)]
        peers += [self.device(self.first, (self.second + d) % self.side) for d in range(1, self.side)]
        return [*peers, self.partner()]

    def greet(self):
        for peer in self.peers():
            pl.semaphore_signal(pltpu.get_barrier_semaphore(), inc=1, device_id=peer, device_id_type=MESH)

    def meet(self):
        pl.semaphore_wait(pltpu.get_barrier_semaphore(), 2 * self.side - 1)


def far_first(side):
    return sorted(range(1, side), key=lambda d: -min(d, side - d))


def remote(src, dst, send_sem, recv_sem, device):
    return pltpu.make_async_remote_copy(src_ref=src, dst_ref=dst, send_sem=send_sem, recv_sem=recv_sem, device_id=device, device_id_type=MESH)


def norm_rows(r_ref, gain, shift, buf, tile):
    rows = pl.ds(pl.multiple_of(tile * TILE, TILE), TILE)
    v = r_ref[rows, :].astype(F32)
    mean = jnp.mean(v, axis=-1, keepdims=True)
    v = v - mean
    var = jnp.mean(v * v, axis=-1, keepdims=True)
    buf[0, rows, :] = (v * lax.rsqrt(var + LN_EPS) * gain + shift).astype(BF16)


class Gather:
    def __init__(self, place, buf, send, recv):
        self.place, self.buf, self.send, self.recv = place, buf, send, recv
        self.half = buf.shape[1] // 2
        self.subs = self.half // TILE
        n = place.chips
        self.next = [place.device(*place.at_pos((place.pos + d) % n))["tp"] for d in (1, n - 1)]

    def hop(self, dr, s, k):
        rows = pl.ds(pl.multiple_of(dr * self.half + k * TILE, TILE), TILE)
        return remote(self.buf.at[s, rows], self.buf.at[s + 1, rows], self.send.at[dr, s, k], self.recv.at[dr, s, k],
                      {"tp": self.next[0] * (1 - dr) + self.next[1] * dr})

    def start(self, norm, before, meanwhile):
        norm(0)
        norm(self.subs)
        self.place.meet()
        before()

        def step(k, carry):
            norm(k)
            norm(self.subs + k)
            for dr in range(2):
                self.hop(dr, 0, k - 1).start()
            return carry
        lax.fori_loop(1, self.subs, step, 0)
        meanwhile()
        for dr in range(2):
            self.hop(dr, 0, self.subs - 1).start()

    def take(self, s, k):
        for dr in range(2):
            self.hop(dr, s - 1, k).wait_recv()

            @pl.when(s < self.place.chips - 1)
            def _():
                self.hop(dr, s, k).start()

    def sent(self, s):
        @pl.when(s < self.place.chips - 1)
        def _():
            for dr in range(2):
                for k in range(self.subs):
                    self.hop(dr, s, k).wait_send()

    def run(self, part):
        n = self.place.chips // 2
        for k in range(self.subs):
            self.take(1, k)

        def step(j, carry):
            for h in range(2):
                for k in range(self.subs):
                    @pl.when(j < n)
                    def _():
                        self.take(2 * j + h, k)
                    part(j - 1, h * self.subs + k)
            return carry
        lax.fori_loop(1, n + 1, step, 0)


class Scatter:
    def __init__(self, place, buf, r1, sums, mid, r2, s1_send, s1_recv, mid_send, mid_recv, s2_send, s2_recv):
        self.place, self.buf, self.r1, self.sums, self.mid, self.r2 = place, buf, r1, sums, mid, r2
        self.mid_send, self.mid_recv = mid_send, mid_recv
        self.s1_send, self.s1_recv, self.s2_send, self.s2_recv = s1_send, s1_recv, s2_send, s2_recv
        self.half = buf.shape[1] // 2

    def rows(self, dr):
        return pl.ds(dr * self.half, self.half)

    def first_copy(self, slot, dr, j, first, second):
        p = self.place
        return remote(self.buf.at[slot, self.rows(dr)], self.r1.at[j, second, self.rows(dr)], self.s1_send.at[j, second, dr],
                      self.s1_recv.at[j, second, dr], p.device(first, p.second))

    def send_rows(self, d, dr, begin, end):
        p = self.place
        second = (p.second + d) % p.side
        for away in far_first(p.side):
            first = (p.first + away) % p.side
            slot = self.slot_of(first, second, dr)

            @pl.when((slot >= begin) & (slot < end))
            def _():
                self.first_copy(slot, dr, p.side - 1 - away, first, second).start()

    def slot_of(self, first, second, dr):
        p = self.place
        pos = p.pos_of(first, second)
        return (p.pos + p.chips - pos) % p.chips if dr == 0 else (pos + p.chips - p.pos) % p.chips

    def arrived(self, second, dr):
        for j in range(self.place.side - 1):
            self.first_copy(0, dr, j, self.place.first, second).wait_recv()

    def total(self, second, dr, rows):
        v = self.buf[self.slot_of(self.place.first, second, dr), rows, :].astype(F32)
        for j in range(self.place.side - 1):
            v = v + self.r1[j, second, rows, :].astype(F32)
        return v

    def tile(self, dr, k):
        return pl.ds(pl.multiple_of(dr * self.half + k * TILE, TILE), TILE)

    def mid_copy(self, dr, k):
        p = self.place
        step = 1 if dr == 0 else p.side - 1
        rows = self.tile(dr, k)
        return remote(self.sums.at[1, rows], self.mid.at[rows], self.mid_send.at[dr, k], self.mid_recv.at[dr, k],
                      p.device(p.first, (p.second + step) % p.side))

    def end_copy(self, d, dr, k):
        p = self.place
        at = 0 if d == 1 else 1
        rows = self.tile(dr, k)
        return remote(self.sums.at[d - 1, rows], self.r2.at[at, rows], self.s2_send.at[at, dr, k], self.s2_recv.at[at, dr, k],
                      p.device(p.first, (p.second + d) % p.side))

    def add(self, d, dr, k, with_mid):
        second = (self.place.second + d) % self.place.side
        rows = self.tile(dr, k)
        v = self.total(second, dr, rows)
        if with_mid:
            self.mid_copy(dr, k).wait_recv()
            v = v + self.mid[rows, :]
        self.sums[d - 1, rows, :] = v

    def tiles(self, fn):
        def one(k, carry):
            fn(k)
            return carry
        lax.fori_loop(0, self.half // TILE, one, 0)

    def finish(self, res, bias, out_ref):
        p = self.place

        def pieces(group, with_mid, copy):
            for d, dr in group:
                self.arrived((p.second + d) % p.side, dr)

            def one(k):
                for d, dr in group:
                    self.add(d, dr, k, with_mid)
                    copy(d, dr, k).start()
            self.tiles(one)

        ends = [(1, 1), (p.side - 1, 0)] if p.side > 2 else [(1, 0), (1, 1)]
        pieces(ends, False, self.end_copy)
        if p.side > 2:
            pieces([(2, 0), (2, 1)], False, lambda d, dr, k: self.mid_copy(dr, k))
            more = [(1, 0), (p.side - 1, 1)]
            pieces(more, True, self.end_copy)
            ends = ends + more
        for dr in range(2):
            self.arrived(p.second, dr)

        def last(k):
            for dr in range(2):
                rows = self.tile(dr, k)
                for d, half in ends:
                    if half == dr:
                        self.end_copy(d, dr, k).wait_recv()
                v = self.total(p.second, dr, rows)
                for j in range(self.r2.shape[0]):
                    v = v + self.r2[j, rows, :]
                out_ref[rows, :] = (res[rows, :] + v + bias).astype(out_ref.dtype)
        self.tiles(last)

        def sent(k):
            if p.side > 2:
                for dr in range(2):
                    self.mid_copy(dr, k).wait_send()
            for d, dr in ends:
                self.end_copy(d, dr, k).wait_send()
        self.tiles(sent)
        for dr in range(2):
            for j in range(p.side - 1):
                for second in range(p.side):
                    self.first_copy(0, dr, j, p.first, second).wait_send()


class Share:
    def __init__(self, place, pairs, local, send, recv):
        self.place, self.pairs, self.local, self.send, self.recv = place, pairs, local, send, recv

    def load(self, i):
        src, own, _ = self.pairs[i]
        return pltpu.make_async_copy(src, own, self.local.at[i])

    def give(self, i):
        _, own, other = self.pairs[i]
        return remote(own, other, self.send.at[i], self.recv.at[i], self.place.partner())


def layer_kernel(group_size, layer, n_seq, r_ref, norm_ref, bout_ref, bdown_ref, bup_ref, wqkv_ref, wout_ref, wup_ref, wdown_ref, out_ref,
                 buf, wu, wd, bu, u, r1, sums, mid, r2, qkv, kvp, w4, res,
                 wl, ws, wr, free, ag_send, ag_recv, ag2_send, ag2_recv, kv_send, kv_recv, a_send, a_recv, f_send, f_recv, w4_send, w4_recv,
                 p_send, p_recv, s_send, s_recv, s1_send, s1_recv, mid_send, mid_recv, s2_send, s2_recv):
    place = Place(group_size)
    slots, block, model = buf.shape
    side, hd, ff = place.side, w4.shape[1] // 2, wup_ref.shape[2]
    n_chunks, per_seq, width = block // TILE, block // n_seq, model // place.side
    per_row = side
    every = slots * TILE
    share = Share(place, [(wout_ref.at[layer], wd.at[pl.ds(0, hd)], wd.at[pl.ds(hd, hd)])]
                  + [(wqkv_ref.at[layer, t], wu.at[:, pl.ds(t * hd, hd)], wu.at[:, pl.ds((3 + t) * hd, hd)]) for t in range(3)]
                  + [(bup_ref.at[pl.ds(layer, 1)], bu.at[:, pl.ds(0, ff)], bu.at[:, pl.ds(ff, ff)]),
                     (wup_ref.at[layer], wu.at[:, pl.ds(0, ff)], wu.at[:, pl.ds(ff, ff)]),
                     (wdown_ref.at[layer], wd.at[pl.ds(0, ff)], wd.at[pl.ds(ff, ff)])], wl, ws, wr)
    area = [2 * hd + i * every for i in range(3)]

    def piece(i, n):
        return wd.at[pl.ds(area[i], every), pl.ds(pl.multiple_of(n * 2 * hd, 2 * hd), 2 * hd)]

    def heads(j, chunk):
        return (piece(2, chunk), piece(2, n_chunks + chunk), piece(1, n_chunks + chunk), piece(1, chunk))[j]

    def partial(chunk):
        over = chunk // per_row
        row = pl.multiple_of(area[0] + every * over * (chunk - per_row + 1), TILE)
        col = pl.multiple_of(width * (chunk * (1 - over) + (per_row - 1) * over), width)
        return row, pl.ds(col, width)

    def cell(chunk):
        return chunk // per_row, pl.ds(pl.multiple_of(chunk % per_row * width, width), width)

    place.greet()
    for i in range(4):
        share.load(i).start()
    gather = Gather(place, buf, ag_send, ag_recv)

    def norm(tile):
        norm_rows(r_ref, norm_ref[layer, 0:1, :], norm_ref[layer, 1:2, :], buf, tile)

    def col(first):
        return pl.ds(pl.multiple_of(first * width, width), width)

    def w_copy(d, h):
        first = (place.first + d) % side
        rows = pl.ds(h * hd, hd)
        return remote(wd.at[rows, col(first)], w4.at[side - 1 - d, rows], w4_send.at[side - 1 - d, h], w4_recv.at[side - 1 - d, h],
                      place.device(first, place.second))

    def share_out():
        share.load(0).wait()
        share.give(0).start()
        for d in far_first(side):
            w_copy(d, 0).start()

    def share_qkv():
        for i in range(1, 4):
            share.load(i).wait()
            share.give(i).start()
    gather.start(norm, share_out, share_qkv)
    share.give(0).wait_recv()
    for d in far_first(side):
        w_copy(d, 1).start()

    def kv_copy(j, h):
        pair = pl.ds(2 * j, 2)
        return remote(qkv.at[pair, :, pl.ds(3 * hd * h + hd, 2 * hd)], kvp.at[pair, :, pl.ds(2 * hd * (1 - h), 2 * hd)],
                      kv_send.at[j, h], kv_recv.at[j, h], place.partner())

    def qkv_part(j, i):
        if i % 2 == 0:
            if i == 0:
                @pl.when(j == 0)
                def _():
                    for t in range(3):
                        share.give(1 + t).wait_recv()
            cols = pl.ds(i // 2 * 2 * hd, 2 * hd)
            rows = buf[pl.ds(2 * j, 2)].reshape(2 * block, model)
            qkv[pl.ds(2 * j, 2), :, cols] = jnp.dot(rows, wu[:, cols], preferred_element_type=F32).astype(BF16).reshape(2, block, 2 * hd)
        if i == 5:
            for h in range(2):
                kv_copy(j, h).start()
            gather.sent(2 * j)
            gather.sent(2 * j + 1)
    gather.run(qkv_part)
    for j in range(slots // 2):
        for h in range(2):
            kv_copy(j, h).wait_recv()
    for i in range(1, 4):
        share.give(i).wait_send()
    for i in (4, 5):
        share.load(i).start()

    nk = slots * per_seq

    def rows_of(chunk):
        return pl.ds(pl.multiple_of(chunk * TILE, TILE), TILE)

    def attend(chunk):
        seq = chunk * TILE // per_seq
        lower = chunk * TILE // (block // 2)
        keys = pl.ds(pl.multiple_of(seq * per_seq, per_seq), per_seq)

        def head_of(h, carry):
            def cols(base, k):
                return pl.ds(pl.multiple_of(h * base + k * hd, hd), hd)
            q = qkv[:, rows_of(chunk), cols(3 * hd, 0)].reshape(every, hd)
            k0 = qkv[:, keys, cols(3 * hd, 1)].reshape(nk, hd)
            v0 = qkv[:, keys, cols(3 * hd, 2)].reshape(nk, hd)
            k1 = kvp[:, keys, cols(2 * hd, 0)].reshape(nk, hd)
            v1 = kvp[:, keys, cols(2 * hd, 1)].reshape(nk, hd)
            dims = (((1,), (1,)), ((), ()))
            s0 = lax.dot_general(q, k0, dims, preferred_element_type=F32) * hd ** -0.5
            s1 = lax.dot_general(q, k1, dims, preferred_element_type=F32) * hd ** -0.5
            top = jnp.maximum(jnp.max(s0, axis=-1, keepdims=True), jnp.max(s1, axis=-1, keepdims=True))
            e0 = jnp.exp(s0 - top)
            e1 = jnp.exp(s1 - top)
            inv = 1.0 / (jnp.sum(e0, axis=-1, keepdims=True) + jnp.sum(e1, axis=-1, keepdims=True))
            a = jnp.dot((e0 * inv).astype(BF16), v0, preferred_element_type=F32)
            a = (a + jnp.dot((e1 * inv).astype(BF16), v1, preferred_element_type=F32)).astype(BF16)
            for slot in range(slots):
                pos = (place.pos + (slots - slot) * (1 - lower) + slot * lower) % slots
                wd[pl.ds(pl.multiple_of(area[1] + pos * TILE, TILE), TILE),
                   pl.ds(pl.multiple_of(chunk * 2 * hd + h * hd, hd), hd)] = a[slot * TILE:(slot + 1) * TILE]
            return carry
        lax.fori_loop(0, 2, head_of, 0)
        for d in near:
            a_copy(chunk, d).start()

    near = (1, side - 1)

    def a_copy(chunk, d):
        return remote(heads(side - 1, chunk), heads(side - 1 - d, chunk), a_send.at[chunk, d // 2], a_recv.at[chunk, d // 2],
                      place.device((place.first + d) % side, place.second))

    def f_copy(chunk, h):
        cols = pl.ds(h * hd, hd)
        return remote(heads(2 - 2 * h, chunk).at[:, cols], heads(1, chunk).at[:, cols], f_send.at[chunk, h], f_recv.at[chunk, h],
                      place.device((place.first + (1 if h == 0 else side - 1)) % side, place.second))

    def forward(chunk):
        for d in near:
            a_copy(chunk, d).wait_recv()
        for h in range(2):
            f_copy(chunk, h).start()

        @pl.when(chunk == 0)
        def _():
            for i in (4, 5):
                share.load(i).wait()
                share.give(i).start()

    def p_copy(chunk, d):
        second = (place.second + d) % side
        row, cols = partial(chunk)
        at, there = cell(chunk)
        return remote(wd.at[pl.ds(pl.multiple_of(row + second * side * TILE, TILE), side * TILE), cols],
                      r1.at[side - 1 - d, at, pl.ds(0, side * TILE), there], p_send.at[chunk, side - 1 - d], p_recv.at[chunk, side - 1 - d],
                      place.device(place.first, second))

    def project(chunk):
        @pl.when(chunk == 0)
        def _():
            for d in range(1, side):
                for h in range(2):
                    w_copy(d, h).wait_recv()
        for h in range(2):
            f_copy(chunk, h).wait_recv()
        half = width // 2
        row, cols = partial(chunk)
        for c in range(2):
            own = pl.ds(pl.multiple_of(place.first * width + c * half, half), half)
            v = jnp.dot(heads(side - 1, chunk)[...], wd[pl.ds(0, 2 * hd), own], preferred_element_type=F32)
            for j in range(side - 1):
                v = v + jnp.dot(heads(j, chunk)[...], w4[j, :, pl.ds(c * half, half)], preferred_element_type=F32)
            wd[pl.ds(row, every), pl.ds(pl.multiple_of(cols.start + c * half, half), half)] = v.astype(BF16)
        for d in far_first(side):
            p_copy(chunk, d).start()

    def s_copy(chunk, d):
        first = (place.first + d) % side
        at, there = cell(chunk)
        i = (first + place.second) % side
        return remote(sums.at[at, pl.ds(pl.multiple_of(i * TILE, TILE), TILE), there],
                      r2.at[0, rows_of(chunk), pl.ds((side - 1 - d) * width, width)], s_send.at[chunk, side - 1 - d], s_recv.at[chunk, side - 1 - d],
                      place.device(first, place.second))

    def add(chunk):
        for d in range(1, side):
            p_copy(chunk, d).wait_recv()
        row, cols = partial(chunk)
        at, there = cell(chunk)

        def one(i, carry):
            rows = rows_of(i)
            v = wd[pl.ds(pl.multiple_of(row + (place.second * side + i) * TILE, TILE), TILE), cols].astype(F32)
            for j in range(side - 1):
                v = v + r1[j, at, rows, there].astype(F32)
            sums[at, rows, there] = v
            return carry
        lax.fori_loop(0, side, one, 0)
        for d in far_first(side):
            s_copy(chunk, d).start()

    gather2 = Gather(place, buf, ag2_send, ag2_recv)
    subs = gather2.subs

    def output(chunk):
        rows = rows_of(chunk)
        at, there = cell(chunk)

        def put(first, v):
            res[rows, col(first)] = r_ref[rows, col(first)].astype(F32) + v + bout_ref[pl.ds(layer, 1), col(first)]
        put(place.first, sums[at, pl.ds(pl.multiple_of((place.first + place.second) % side * TILE, TILE), TILE), there])
        for j in range(side - 1):
            s_copy(chunk, side - 1 - j).wait_recv()
            put((place.first + 1 + j) % side, r2[0, rows, pl.ds(j * width, width)])
        norm_rows(res, norm_ref[layer, 2:3, :], norm_ref[layer, 3:4, :], buf, chunk)

        @pl.when(chunk > 0)
        def _():
            gather2.hop((chunk - 1) // subs, 0, (chunk - 1) % subs).start()

    lag = n_chunks // 2
    stages = ((attend, 0), (forward, lag - 1), (project, lag), (add, lag + 1), (output, lag + 2))

    def step(i, carry):
        for stage, at in stages:
            @pl.when((i >= at) & (i < at + n_chunks))
            def _():
                stage(i - at)
        return carry
    lax.fori_loop(0, n_chunks + lag + 2, step, 0)

    def done(chunk, carry):
        for d in range(1, side):
            p_copy(chunk, d).wait_send()
            s_copy(chunk, d).wait_send()
        for d in near:
            a_copy(chunk, d).wait_send()
        for h in range(2):
            f_copy(chunk, h).wait_send()
        return carry
    lax.fori_loop(0, n_chunks, done, 0)
    gather2.hop(1, 0, subs - 1).start()
    for d in range(1, side):
        for h in range(2):
            w_copy(d, h).wait_send()
    share.give(0).wait_send()
    share.load(6).start()
    pl.semaphore_signal(free, inc=1, device_id=place.partner(), device_id_type=MESH)
    for j in range(slots // 2):
        for h in range(2):
            kv_copy(j, h).wait_send()

    scatter = Scatter(place, buf, r1, sums, mid, r2, s1_send, s1_recv, mid_send, mid_recv, s2_send, s2_recv)
    up_w, down_w = ff // 2, model // 4

    def up(j, c):
        rows = buf[pl.ds(2 * j, 2)].reshape(2 * block, model)
        cols = pl.ds(c * up_w, up_w)
        hidden = jnp.dot(rows, wu[:, cols], preferred_element_type=F32) + bu[:, cols]
        u[:, cols] = jax.nn.gelu(hidden, approximate=True).astype(BF16)

    def down(j, c):
        cols = pl.ds(c * down_w, down_w)
        buf[pl.ds(2 * j, 2), :, cols] = jnp.dot(u[...], wd[:, cols], preferred_element_type=F32).astype(BF16).reshape(2, block, down_w)

    def mlp_part(j, i):
        if i == 0:
            @pl.when(j == 0)
            def _():
                share.load(6).wait()
                pl.semaphore_wait(free, 1)
                share.give(6).start()
                share.give(4).wait_recv()
                share.give(5).wait_recv()

            @pl.when(j == slots // 2 - 1)
            def _():
                for d, dr in ((1, 1), (3, 0), (2, 0), (2, 1), (1, 0), (3, 1)):
                    scatter.send_rows(d, dr, 0, slots - 2)
            up(j, 0)
            up(j, 1)
        elif i == 1:
            up(j, 2)
        elif i == 2:
            up(j, 3)
        elif i == 3:
            @pl.when(j == 0)
            def _():
                share.give(6).wait_recv()
            gather2.sent(2 * j)
            gather2.sent(2 * j + 1)
            down(j, 0)
        elif i == 4:
            down(j, 1)
        else:
            down(j, 2)
            down(j, 3)
    gather2.run(mlp_part)
    for d, dr in ((1, 0), (3, 1)):
        scatter.send_rows(d, dr, slots - 2, slots)
    for dr in range(2):
        scatter.send_rows(0, dr, 0, slots)
    scatter.finish(res, bdown_ref[pl.ds(layer, 1), :], out_ref)
    for i in (4, 5, 6):
        share.give(i).wait_send()


def solution(mesh):
    group_size = mesh.shape["tp"]
    side = math.isqrt(group_size // 2)
    chips = side * side
    dma = pltpu.SemaphoreType.DMA
    vmem = pl.BlockSpec(memory_space=pltpu.VMEM)
    hbm = pl.BlockSpec(memory_space=pl.ANY)

    def local_layers(hidden_in, norms, w_qkv, w_out, b_out, w_up, b_up, w_down, b_down):
        n_seq, per_seq, model = hidden_in.shape
        n_layers, head_dim, ff = w_qkv.shape[0], w_qkv.shape[-1], w_up.shape[-1]
        block = n_seq * per_seq
        subs = block // 2 // TILE
        n_chunks = block // TILE
        residual = hidden_in.reshape(block, model)
        w_qkv = w_qkv.transpose(0, 2, 3, 1, 4).reshape(n_layers, 3, model, head_dim)
        w_out = w_out.reshape(n_layers, head_dim, model)
        for layer in range(n_layers):
            residual = pl.pallas_call(
                functools.partial(layer_kernel, group_size, layer, n_seq), name=f"layer{layer}",
                out_shape=jax.ShapeDtypeStruct((block, model), F32 if layer < n_layers - 1 else BF16),
                in_specs=[vmem] * 4 + [hbm] * 5, out_specs=vmem,
                scratch_shapes=[
                    pltpu.VMEM((chips, block, model), BF16), pltpu.VMEM((model, 2 * ff), BF16), pltpu.VMEM((2 * ff, model), BF16),
                    pltpu.VMEM((1, 2 * ff), F32), pltpu.VMEM((2 * block, 2 * ff), BF16), pltpu.VMEM((side - 1, side, block, model), BF16),
                    pltpu.VMEM((side - 1, block, model), F32), pltpu.VMEM((block, model), F32), pltpu.VMEM((2, block, model), F32),
                    pltpu.VMEM((chips, block, 6 * head_dim), BF16), pltpu.VMEM((chips, block, 4 * head_dim), BF16),
                    pltpu.VMEM((side - 1, 2 * head_dim, model // side), BF16), pltpu.VMEM((block, model), F32),
                    *[dma((7,))] * 3, pltpu.SemaphoreType.REGULAR, *[dma((2, chips - 1, subs))] * 4, *[dma((chips // 2, 2))] * 2,
                    *[dma((n_chunks, 2))] * 4, *[dma((side - 1, 2))] * 2, *[dma((n_chunks, side - 1))] * 4,
                    *[dma((side - 1, side, 2))] * 2, *[dma((2, subs))] * 2, *[dma((2, 2, subs))] * 2],
                compiler_params=pltpu.CompilerParams(collective_id=layer, has_side_effects=True, vmem_limit_bytes=VMEM_LIMIT),
            )(residual, norms, b_out, b_down, b_up, w_qkv, w_out, w_up, w_down)
        return residual.reshape(n_seq, per_seq, model)

    in_specs = (P('dp', 'tp', None), P(), P(None, None, None, 'tp', None), P(None, 'tp', None, None), P(), P(None, None, 'tp'), P(None, 'tp'), P(None, 'tp', None), P())
    return jax.shard_map(local_layers, mesh=mesh, in_specs=in_specs, out_specs=P('dp', 'tp', None), check_vma=False)
```

```python
import functools
import math

import jax
import jax.numpy as jnp
from jax import lax
from jax.experimental import pallas as pl
from jax.experimental.pallas import tpu as pltpu
from jax.sharding import PartitionSpec as P

LN_EPS = 1e-5
MESH = pl.DeviceIdType.MESH
F32 = jnp.float32
BF16 = jnp.bfloat16
VMEM_LIMIT = 66_900_000
TILE = 16


class Place:
    def __init__(self, group_size):
        self.side = side = math.isqrt(group_size // 2)
        self.chips = side * side
        index = lax.axis_index("tp")
        self.core = index % 2
        chip = index // 2
        x, y = chip % side, chip // side
        self.first = x * (1 - self.core) + y * self.core
        self.second = y * (1 - self.core) + x * self.core
        self.pos = self.pos_of(self.first, self.second)

    def device(self, first, second):
        x = first * (1 - self.core) + second * self.core
        y = second * (1 - self.core) + first * self.core
        return {"tp": (y * self.side + x) * 2 + self.core}

    def partner(self):
        x = self.first * (1 - self.core) + self.second * self.core
        y = self.second * (1 - self.core) + self.first * self.core
        return {"tp": (y * self.side + x) * 2 + 1 - self.core}

    def pos_of(self, first, second):
        return second * self.side + (first + second) % self.side

    def at_pos(self, pos):
        second = pos // self.side
        return (pos % self.side + self.side - second) % self.side, second

    def peers(self):
        peers = [self.device((self.first + d) % self.side, self.second) for d in range(1, self.side)]
        peers += [self.device(self.first, (self.second + d) % self.side) for d in range(1, self.side)]
        return [*peers, self.partner()]

    def greet(self):
        for peer in self.peers():
            pl.semaphore_signal(pltpu.get_barrier_semaphore(), inc=1, device_id=peer, device_id_type=MESH)

    def meet(self):
        pl.semaphore_wait(pltpu.get_barrier_semaphore(), 2 * self.side - 1)


def far_first(side):
    return sorted(range(1, side), key=lambda d: -min(d, side - d))


def remote(src, dst, send_sem, recv_sem, device):
    return pltpu.make_async_remote_copy(src_ref=src, dst_ref=dst, send_sem=send_sem, recv_sem=recv_sem, device_id=device, device_id_type=MESH)


def norm_rows(r_ref, gain, shift, buf, tile):
    rows = pl.ds(pl.multiple_of(tile * TILE, TILE), TILE)
    v = r_ref[rows, :].astype(F32)
    mean = jnp.mean(v, axis=-1, keepdims=True)
    v = v - mean
    var = jnp.mean(v * v, axis=-1, keepdims=True)
    buf[0, rows, :] = (v * lax.rsqrt(var + LN_EPS) * gain + shift).astype(BF16)


class Gather:
    def __init__(self, place, buf, send, recv):
        self.place, self.buf, self.send, self.recv = place, buf, send, recv
        self.half = buf.shape[1] // 2
        self.subs = self.half // TILE
        n = place.chips
        self.next = [place.device(*place.at_pos((place.pos + d) % n))["tp"] for d in (1, n - 1)]

    def hop(self, dr, s, k):
        rows = pl.ds(pl.multiple_of(dr * self.half + k * TILE, TILE), TILE)
        return remote(self.buf.at[s, rows], self.buf.at[s + 1, rows], self.send.at[dr, s, k], self.recv.at[dr, s, k],
                      {"tp": self.next[0] * (1 - dr) + self.next[1] * dr})

    def start(self, norm, before, meanwhile):
        norm(0)
        norm(self.subs)
        self.place.meet()
        before()

        def step(k, carry):
            norm(k)
            norm(self.subs + k)
            for dr in range(2):
                self.hop(dr, 0, k - 1).start()
            return carry
        lax.fori_loop(1, self.subs, step, 0)
        meanwhile()
        for dr in range(2):
            self.hop(dr, 0, self.subs - 1).start()

    def take(self, s, k):
        for dr in range(2):
            self.hop(dr, s - 1, k).wait_recv()

            @pl.when(s < self.place.chips - 1)
            def _():
                self.hop(dr, s, k).start()

    def sent(self, s):
        @pl.when(s < self.place.chips - 1)
        def _():
            for dr in range(2):
                for k in range(self.subs):
                    self.hop(dr, s, k).wait_send()

    def run(self, part):
        n = self.place.chips // 2
        for k in range(self.subs):
            self.take(1, k)

        def step(j, carry):
            for h in range(2):
                for k in range(self.subs):
                    @pl.when(j < n)
                    def _():
                        self.take(2 * j + h, k)
                    part(j - 1, h * self.subs + k)
            return carry
        lax.fori_loop(1, n + 1, step, 0)


class Scatter:
    def __init__(self, place, buf, r1, sums, mid, r2, s1_send, s1_recv, mid_send, mid_recv, s2_send, s2_recv):
        self.place, self.buf, self.r1, self.sums, self.mid, self.r2 = place, buf, r1, sums, mid, r2
        self.mid_send, self.mid_recv = mid_send, mid_recv
        self.s1_send, self.s1_recv, self.s2_send, self.s2_recv = s1_send, s1_recv, s2_send, s2_recv
        self.half = buf.shape[1] // 2

    def rows(self, dr):
        return pl.ds(dr * self.half, self.half)

    def first_copy(self, slot, dr, j, first, second):
        p = self.place
        return remote(self.buf.at[slot, self.rows(dr)], self.r1.at[j, second, self.rows(dr)], self.s1_send.at[j, second, dr],
                      self.s1_recv.at[j, second, dr], p.device(first, p.second))

    def send_rows(self, d, dr, begin, end):
        p = self.place
        second = (p.second + d) % p.side
        for away in far_first(p.side):
            first = (p.first + away) % p.side
            slot = self.slot_of(first, second, dr)

            @pl.when((slot >= begin) & (slot < end))
            def _():
                self.first_copy(slot, dr, p.side - 1 - away, first, second).start()

    def slot_of(self, first, second, dr):
        p = self.place
        pos = p.pos_of(first, second)
        return (p.pos + p.chips - pos) % p.chips if dr == 0 else (pos + p.chips - p.pos) % p.chips

    def arrived(self, second, dr):
        for j in range(self.place.side - 1):
            self.first_copy(0, dr, j, self.place.first, second).wait_recv()

    def total(self, second, dr, rows):
        v = self.buf[self.slot_of(self.place.first, second, dr), rows, :].astype(F32)
        for j in range(self.place.side - 1):
            v = v + self.r1[j, second, rows, :].astype(F32)
        return v

    def tile(self, dr, k):
        return pl.ds(pl.multiple_of(dr * self.half + k * TILE, TILE), TILE)

    def mid_copy(self, dr, k):
        p = self.place
        step = 1 if dr == 0 else p.side - 1
        rows = self.tile(dr, k)
        return remote(self.sums.at[1, rows], self.mid.at[rows], self.mid_send.at[dr, k], self.mid_recv.at[dr, k],
                      p.device(p.first, (p.second + step) % p.side))

    def end_copy(self, d, dr, k):
        p = self.place
        at = 0 if d == 1 else 1
        rows = self.tile(dr, k)
        return remote(self.sums.at[d - 1, rows], self.r2.at[at, rows], self.s2_send.at[at, dr, k], self.s2_recv.at[at, dr, k],
                      p.device(p.first, (p.second + d) % p.side))

    def add(self, d, dr, k, with_mid):
        second = (self.place.second + d) % self.place.side
        rows = self.tile(dr, k)
        v = self.total(second, dr, rows)
        if with_mid:
            self.mid_copy(dr, k).wait_recv()
            v = v + self.mid[rows, :]
        self.sums[d - 1, rows, :] = v

    def tiles(self, fn):
        def one(k, carry):
            fn(k)
            return carry
        lax.fori_loop(0, self.half // TILE, one, 0)

    def finish(self, res, bias, out_ref, meanwhile):
        p = self.place

        def pieces(group, with_mid, copy):
            for d, dr in group:
                self.arrived((p.second + d) % p.side, dr)

            def one(k):
                for d, dr in group:
                    self.add(d, dr, k, with_mid)
                    copy(d, dr, k).start()
            self.tiles(one)

        ends = [(1, 1), (p.side - 1, 0)] if p.side > 2 else [(1, 0), (1, 1)]
        pieces(ends, False, self.end_copy)
        if p.side > 2:
            pieces([(2, 0), (2, 1)], False, lambda d, dr, k: self.mid_copy(dr, k))
            more = [(1, 0), (p.side - 1, 1)]
            pieces(more, True, self.end_copy)
            ends = ends + more
        meanwhile()
        for dr in range(2):
            self.arrived(p.second, dr)

        def last(k):
            for dr in range(2):
                rows = self.tile(dr, k)
                for d, half in ends:
                    if half == dr:
                        self.end_copy(d, dr, k).wait_recv()
                v = self.total(p.second, dr, rows)
                for j in range(self.r2.shape[0]):
                    v = v + self.r2[j, rows, :]
                v = res[rows, :] + v + bias
                res[rows, :] = v
                out_ref[rows, :] = v.astype(out_ref.dtype)
        self.tiles(last)

        def sent(k):
            if p.side > 2:
                for dr in range(2):
                    self.mid_copy(dr, k).wait_send()
            for d, dr in ends:
                self.end_copy(d, dr, k).wait_send()
        self.tiles(sent)
        for dr in range(2):
            for j in range(p.side - 1):
                for second in range(p.side):
                    self.first_copy(0, dr, j, p.first, second).wait_send()


class Share:
    def __init__(self, place, pairs, local, send, recv):
        self.place, self.pairs, self.local, self.send, self.recv = place, pairs, local, send, recv

    def load(self, i):
        src, own, _ = self.pairs[i]
        return pltpu.make_async_copy(src, own, self.local.at[i])

    def give(self, i):
        _, own, other = self.pairs[i]
        return remote(own, other, self.send.at[i], self.recv.at[i], self.place.partner())


def layers_kernel(group_size, n_seq, r_ref, norm_ref, bout_ref, bdown_ref, bup_ref, wqkv_ref, wout_ref, wup_ref, wdown_ref, out_ref,
                 buf, wu, wd, bu, u, r1, sums, mid, r2, qkv, kvp, wo, w4, res,
                 wl, ws, wr, free, ag_send, ag_recv, ag2_send, ag2_recv, kv_send, kv_recv, a_send, a_recv, f_send, f_recv, w4_send, w4_recv,
                 p_send, p_recv, s_send, s_recv, s1_send, s1_recv, mid_send, mid_recv, s2_send, s2_recv):
    place = Place(group_size)
    slots, block, model = buf.shape
    side, hd, ff = place.side, w4.shape[1] // 2, wup_ref.shape[2]
    n_chunks, per_seq, width = block // TILE, block // n_seq, model // place.side
    per_row = side
    every = slots * TILE

    def widen(i, carry):
        rows = pl.ds(pl.multiple_of(i * TILE, TILE), TILE)
        res[rows, :] = r_ref[rows, :].astype(F32)
        return carry
    lax.fori_loop(0, n_chunks, widen, 0)

    def one_layer(layer, carry):
        share = Share(place, [(wout_ref.at[layer], wo.at[pl.ds(0, hd)], wo.at[pl.ds(hd, hd)])]
                      + [(wqkv_ref.at[layer, t], wu.at[:, pl.ds(t * hd, hd)], wu.at[:, pl.ds((3 + t) * hd, hd)]) for t in range(3)]
                      + [(bup_ref, bu.at[:, pl.ds(0, ff)], bu.at[:, pl.ds(ff, ff)]),
                         (wup_ref.at[layer], wu.at[:, pl.ds(0, ff)], wu.at[:, pl.ds(ff, ff)]),
                         (wdown_ref.at[layer], wd.at[pl.ds(0, ff)], wd.at[pl.ds(ff, ff)])], wl, ws, wr)
        area = [2 * hd + i * every for i in range(3)]

        def piece(i, n):
            return wd.at[pl.ds(area[i], every), pl.ds(pl.multiple_of(n * 2 * hd, 2 * hd), 2 * hd)]

        def heads(j, chunk):
            return (piece(2, chunk), piece(2, n_chunks + chunk), piece(1, n_chunks + chunk), piece(1, chunk))[j]

        def partial(chunk):
            over = chunk // per_row
            row = pl.multiple_of(area[0] + every * over * (chunk - per_row + 1), TILE)
            col = pl.multiple_of(width * (chunk * (1 - over) + (per_row - 1) * over), width)
            return row, pl.ds(col, width)

        def cell(chunk):
            return chunk // per_row, pl.ds(pl.multiple_of(chunk % per_row * width, width), width)

        place.greet()
        for i in range(1, 4):
            share.load(i).start()

        @pl.when(layer == 0)
        def _():
            share.load(0).start()
        gather = Gather(place, buf, ag_send, ag_recv)

        def norm(tile):
            norm_rows(res, norm_ref[layer, 0:1, :], norm_ref[layer, 1:2, :], buf, tile)

        def col(first):
            return pl.ds(pl.multiple_of(first * width, width), width)

        def w_copy(d, h):
            first = (place.first + d) % side
            rows = pl.ds(h * hd, hd)
            return remote(wo.at[rows, col(first)], w4.at[side - 1 - d, rows], w4_send.at[side - 1 - d, h], w4_recv.at[side - 1 - d, h],
                          place.device(first, place.second))

        def share_out(which):
            which.load(0).wait()
            which.give(0).start()
            for d in far_first(side):
                w_copy(d, 0).start()

        def share_rest(which):
            which.give(0).wait_recv()
            for d in far_first(side):
                w_copy(d, 1).start()

        def share_qkv():
            for i in range(1, 4):
                share.load(i).wait()
                share.give(i).start()
        gather.start(norm, lambda: pl.when(layer == 0)(lambda: share_out(share)), share_qkv)
        pl.when(layer == 0)(lambda: share_rest(share))

        def kv_copy(j, h):
            pair = pl.ds(2 * j, 2)
            return remote(qkv.at[pair, :, pl.ds(3 * hd * h + hd, 2 * hd)], kvp.at[pair, :, pl.ds(2 * hd * (1 - h), 2 * hd)],
                          kv_send.at[j, h], kv_recv.at[j, h], place.partner())

        def qkv_part(j, i):
            if i % 2 == 0:
                if i == 0:
                    @pl.when(j == 0)
                    def _():
                        for t in range(3):
                            share.give(1 + t).wait_recv()
                cols = pl.ds(i // 2 * 2 * hd, 2 * hd)
                rows = buf[pl.ds(2 * j, 2)].reshape(2 * block, model)
                qkv[pl.ds(2 * j, 2), :, cols] = jnp.dot(rows, wu[:, cols], preferred_element_type=F32).astype(BF16).reshape(2, block, 2 * hd)
            if i == 5:
                for h in range(2):
                    kv_copy(j, h).start()
                gather.sent(2 * j)
                gather.sent(2 * j + 1)
        gather.run(qkv_part)
        for j in range(slots // 2):
            for h in range(2):
                kv_copy(j, h).wait_recv()
        for i in range(1, 4):
            share.give(i).wait_send()
        for i in (4, 5):
            share.load(i).start()

        nk = slots * per_seq

        def rows_of(chunk):
            return pl.ds(pl.multiple_of(chunk * TILE, TILE), TILE)

        def attend(chunk):
            seq = chunk * TILE // per_seq
            lower = chunk * TILE // (block // 2)
            keys = pl.ds(pl.multiple_of(seq * per_seq, per_seq), per_seq)

            def head_of(h, carry):
                def cols(base, k):
                    return pl.ds(pl.multiple_of(h * base + k * hd, hd), hd)
                q = qkv[:, rows_of(chunk), cols(3 * hd, 0)].reshape(every, hd)
                k0 = qkv[:, keys, cols(3 * hd, 1)].reshape(nk, hd)
                v0 = qkv[:, keys, cols(3 * hd, 2)].reshape(nk, hd)
                k1 = kvp[:, keys, cols(2 * hd, 0)].reshape(nk, hd)
                v1 = kvp[:, keys, cols(2 * hd, 1)].reshape(nk, hd)
                dims = (((1,), (1,)), ((), ()))
                s0 = lax.dot_general(q, k0, dims, preferred_element_type=F32) * hd ** -0.5
                s1 = lax.dot_general(q, k1, dims, preferred_element_type=F32) * hd ** -0.5
                top = jnp.maximum(jnp.max(s0, axis=-1, keepdims=True), jnp.max(s1, axis=-1, keepdims=True))
                e0 = jnp.exp(s0 - top)
                e1 = jnp.exp(s1 - top)
                inv = 1.0 / (jnp.sum(e0, axis=-1, keepdims=True) + jnp.sum(e1, axis=-1, keepdims=True))
                a = jnp.dot((e0 * inv).astype(BF16), v0, preferred_element_type=F32)
                a = (a + jnp.dot((e1 * inv).astype(BF16), v1, preferred_element_type=F32)).astype(BF16)
                for slot in range(slots):
                    pos = (place.pos + (slots - slot) * (1 - lower) + slot * lower) % slots
                    wd[pl.ds(pl.multiple_of(area[1] + pos * TILE, TILE), TILE),
                       pl.ds(pl.multiple_of(chunk * 2 * hd + h * hd, hd), hd)] = a[slot * TILE:(slot + 1) * TILE]
                return carry
            lax.fori_loop(0, 2, head_of, 0)
            for d in near:
                a_copy(chunk, d).start()

        near = (1, side - 1)

        def a_copy(chunk, d):
            return remote(heads(side - 1, chunk), heads(side - 1 - d, chunk), a_send.at[chunk, d // 2], a_recv.at[chunk, d // 2],
                          place.device((place.first + d) % side, place.second))

        def f_copy(chunk, h):
            cols = pl.ds(h * hd, hd)
            return remote(heads(2 - 2 * h, chunk).at[:, cols], heads(1, chunk).at[:, cols], f_send.at[chunk, h], f_recv.at[chunk, h],
                          place.device((place.first + (1 if h == 0 else side - 1)) % side, place.second))

        def forward(chunk):
            for d in near:
                a_copy(chunk, d).wait_recv()
            for h in range(2):
                f_copy(chunk, h).start()

            @pl.when(chunk == 0)
            def _():
                for i in (4, 5):
                    share.load(i).wait()
                    share.give(i).start()

        def p_copy(chunk, d):
            second = (place.second + d) % side
            row, cols = partial(chunk)
            at, there = cell(chunk)
            return remote(wd.at[pl.ds(pl.multiple_of(row + second * side * TILE, TILE), side * TILE), cols],
                          r1.at[side - 1 - d, at, pl.ds(0, side * TILE), there], p_send.at[chunk, side - 1 - d], p_recv.at[chunk, side - 1 - d],
                          place.device(place.first, second))

        def project(chunk):
            @pl.when(chunk == 0)
            def _():
                for d in range(1, side):
                    for h in range(2):
                        w_copy(d, h).wait_recv()
            for h in range(2):
                f_copy(chunk, h).wait_recv()
            half = width // 2
            row, cols = partial(chunk)
            for c in range(2):
                own = pl.ds(pl.multiple_of(place.first * width + c * half, half), half)
                v = jnp.dot(heads(side - 1, chunk)[...], wo[:, own], preferred_element_type=F32)
                for j in range(side - 1):
                    v = v + jnp.dot(heads(j, chunk)[...], w4[j, :, pl.ds(c * half, half)], preferred_element_type=F32)
                wd[pl.ds(row, every), pl.ds(pl.multiple_of(cols.start + c * half, half), half)] = v.astype(BF16)
            for d in far_first(side):
                p_copy(chunk, d).start()

        def s_copy(chunk, d):
            first = (place.first + d) % side
            at, there = cell(chunk)
            i = (first + place.second) % side
            return remote(sums.at[at, pl.ds(pl.multiple_of(i * TILE, TILE), TILE), there],
                          r2.at[0, rows_of(chunk), pl.ds((side - 1 - d) * width, width)], s_send.at[chunk, side - 1 - d], s_recv.at[chunk, side - 1 - d],
                          place.device(first, place.second))

        def add(chunk):
            for d in range(1, side):
                p_copy(chunk, d).wait_recv()
            row, cols = partial(chunk)
            at, there = cell(chunk)

            def one(i, carry):
                rows = rows_of(i)
                v = wd[pl.ds(pl.multiple_of(row + (place.second * side + i) * TILE, TILE), TILE), cols].astype(F32)
                for j in range(side - 1):
                    v = v + r1[j, at, rows, there].astype(F32)
                sums[at, rows, there] = v
                return carry
            lax.fori_loop(0, side, one, 0)
            for d in far_first(side):
                s_copy(chunk, d).start()

        gather2 = Gather(place, buf, ag2_send, ag2_recv)
        subs = gather2.subs

        def output(chunk):
            rows = rows_of(chunk)
            at, there = cell(chunk)

            def put(first, v):
                res[rows, col(first)] = res[rows, col(first)] + v + bout_ref[pl.ds(layer, 1), col(first)]
            put(place.first, sums[at, pl.ds(pl.multiple_of((place.first + place.second) % side * TILE, TILE), TILE), there])
            for j in range(side - 1):
                s_copy(chunk, side - 1 - j).wait_recv()
                put((place.first + 1 + j) % side, r2[0, rows, pl.ds(j * width, width)])
            norm_rows(res, norm_ref[layer, 2:3, :], norm_ref[layer, 3:4, :], buf, chunk)

            @pl.when(chunk > 0)
            def _():
                gather2.hop((chunk - 1) // subs, 0, (chunk - 1) % subs).start()

        lag = n_chunks // 2
        stages = ((attend, 0), (forward, lag - 1), (project, lag), (add, lag + 1), (output, lag + 2))

        def step(i, carry):
            for stage, at in stages:
                @pl.when((i >= at) & (i < at + n_chunks))
                def _():
                    stage(i - at)
            return carry
        lax.fori_loop(0, n_chunks + lag + 2, step, 0)

        def done(chunk, carry):
            for d in range(1, side):
                p_copy(chunk, d).wait_send()
                s_copy(chunk, d).wait_send()
            for d in near:
                a_copy(chunk, d).wait_send()
            for h in range(2):
                f_copy(chunk, h).wait_send()
            return carry
        lax.fori_loop(0, n_chunks, done, 0)
        gather2.hop(1, 0, subs - 1).start()
        for d in range(1, side):
            for h in range(2):
                w_copy(d, h).wait_send()
        share.give(0).wait_send()
        share.load(6).start()
        pl.semaphore_signal(free, inc=1, device_id=place.partner(), device_id_type=MESH)
        for j in range(slots // 2):
            for h in range(2):
                kv_copy(j, h).wait_send()

        scatter = Scatter(place, buf, r1, sums, mid, r2, s1_send, s1_recv, mid_send, mid_recv, s2_send, s2_recv)
        up_w, down_w = ff // 2, model // 4

        def up(j, c):
            rows = buf[pl.ds(2 * j, 2)].reshape(2 * block, model)
            cols = pl.ds(c * up_w, up_w)
            hidden = jnp.dot(rows, wu[:, cols], preferred_element_type=F32) + bu[pl.ds(layer, 1), cols]
            u[:, cols] = jax.nn.gelu(hidden, approximate=True).astype(BF16)

        def down(j, c):
            cols = pl.ds(c * down_w, down_w)
            buf[pl.ds(2 * j, 2), :, cols] = jnp.dot(u[...], wd[:, cols], preferred_element_type=F32).astype(BF16).reshape(2, block, down_w)

        def mlp_part(j, i):
            if i == 0:
                @pl.when(j == 0)
                def _():
                    share.load(6).wait()
                    pl.semaphore_wait(free, 1)
                    share.give(6).start()
                    share.give(4).wait_recv()
                    share.give(5).wait_recv()

                @pl.when(j == slots // 2 - 1)
                def _():
                    for d, dr in ((1, 1), (3, 0), (2, 0), (2, 1), (1, 0), (3, 1)):
                        scatter.send_rows(d, dr, 0, slots - 2)
                up(j, 0)
                up(j, 1)
            elif i == 1:
                up(j, 2)
            elif i == 2:
                up(j, 3)
            elif i == 3:
                @pl.when(j == 0)
                def _():
                    share.give(6).wait_recv()
                gather2.sent(2 * j)
                gather2.sent(2 * j + 1)
                down(j, 0)
            elif i == 4:
                down(j, 1)
            else:
                down(j, 2)
                down(j, 3)
        gather2.run(mlp_part)
        for d, dr in ((1, 0), (3, 1)):
            scatter.send_rows(d, dr, slots - 2, slots)
        for dr in range(2):
            scatter.send_rows(0, dr, 0, slots)
        following = Share(place, [(wout_ref.at[layer + 1], wo.at[pl.ds(0, hd)], wo.at[pl.ds(hd, hd)])], wl, ws, wr)
        more = pl.when(layer + 1 < wqkv_ref.shape[0])
        more(lambda: following.load(0).start())
        scatter.finish(res, bdown_ref[pl.ds(layer, 1), :], out_ref, lambda: more(lambda: share_out(following)))
        more(lambda: share_rest(following))
        for i in (4, 5, 6):
            share.give(i).wait_send()
        return carry
    lax.fori_loop(0, wqkv_ref.shape[0], one_layer, 0)


def solution(mesh):
    group_size = mesh.shape["tp"]
    side = math.isqrt(group_size // 2)
    chips = side * side
    dma = pltpu.SemaphoreType.DMA
    vmem = pl.BlockSpec(memory_space=pltpu.VMEM)
    hbm = pl.BlockSpec(memory_space=pl.ANY)

    def local_layers(hidden_in, norms, w_qkv, w_out, b_out, w_up, b_up, w_down, b_down):
        n_seq, per_seq, model = hidden_in.shape
        n_layers, head_dim, ff = w_qkv.shape[0], w_qkv.shape[-1], w_up.shape[-1]
        block = n_seq * per_seq
        subs = block // 2 // TILE
        n_chunks = block // TILE
        residual = hidden_in.reshape(block, model)
        w_qkv = w_qkv.transpose(0, 2, 3, 1, 4).reshape(n_layers, 3, model, head_dim)
        w_out = w_out.reshape(n_layers, head_dim, model)
        residual = pl.pallas_call(
            functools.partial(layers_kernel, group_size, n_seq), name="layers",
            out_shape=jax.ShapeDtypeStruct((block, model), BF16),
            in_specs=[vmem] * 4 + [hbm] * 5, out_specs=vmem,
            scratch_shapes=[
                pltpu.VMEM((chips, block, model), BF16), pltpu.VMEM((model, 2 * ff), BF16), pltpu.VMEM((2 * ff, model), BF16),
                pltpu.VMEM((n_layers, 2 * ff), F32), pltpu.VMEM((2 * block, 2 * ff), BF16), pltpu.VMEM((side - 1, side, block, model), BF16),
                pltpu.VMEM((side - 1, block, model), F32), pltpu.VMEM((block, model), F32), pltpu.VMEM((2, block, model), F32),
                pltpu.VMEM((chips, block, 6 * head_dim), BF16), pltpu.VMEM((chips, block, 4 * head_dim), BF16),
                pltpu.VMEM((2 * head_dim, model), BF16), pltpu.VMEM((side - 1, 2 * head_dim, model // side), BF16),
                pltpu.VMEM((block, model), F32),
                *[dma((7,))] * 3, pltpu.SemaphoreType.REGULAR, *[dma((2, chips - 1, subs))] * 4, *[dma((chips // 2, 2))] * 2,
                *[dma((n_chunks, 2))] * 4, *[dma((side - 1, 2))] * 2, *[dma((n_chunks, side - 1))] * 4,
                *[dma((side - 1, side, 2))] * 2, *[dma((2, subs))] * 2, *[dma((2, 2, subs))] * 2],
            compiler_params=pltpu.CompilerParams(collective_id=0, has_side_effects=True, vmem_limit_bytes=VMEM_LIMIT),
        )(residual, norms, b_out, b_down, b_up, w_qkv, w_out, w_up, w_down)
        return residual.reshape(n_seq, per_seq, model)

    in_specs = (P('dp', 'tp', None), P(), P(None, None, None, 'tp', None), P(None, 'tp', None, None), P(), P(None, None, 'tp'), P(None, 'tp'), P(None, 'tp', None), P())
    return jax.shard_map(local_layers, mesh=mesh, in_specs=in_specs, out_specs=P('dp', 'tp', None), check_vma=False)
```

```python
import functools
import math

import jax
import jax.numpy as jnp
from jax import lax
from jax.experimental import pallas as pl
from jax.experimental.pallas import tpu as pltpu
from jax.sharding import PartitionSpec as P

LN_EPS = 1e-5
MESH = pl.DeviceIdType.MESH
F32 = jnp.float32
BF16 = jnp.bfloat16
VMEM_LIMIT = 66_900_000
TILE = 16


class Place:
    def __init__(self, group_size):
        self.side = side = math.isqrt(group_size // 2)
        self.chips = side * side
        index = lax.axis_index("tp")
        self.core = index % 2
        chip = index // 2
        x, y = chip % side, chip // side
        self.first = x * (1 - self.core) + y * self.core
        self.second = y * (1 - self.core) + x * self.core
        self.pos = self.pos_of(self.first, self.second)

    def device(self, first, second):
        x = first * (1 - self.core) + second * self.core
        y = second * (1 - self.core) + first * self.core
        return {"tp": (y * self.side + x) * 2 + self.core}

    def partner(self):
        x = self.first * (1 - self.core) + self.second * self.core
        y = self.second * (1 - self.core) + self.first * self.core
        return {"tp": (y * self.side + x) * 2 + 1 - self.core}

    def pos_of(self, first, second):
        return second * self.side + (first + second) % self.side

    def at_pos(self, pos):
        second = pos // self.side
        return (pos % self.side + self.side - second) % self.side, second

    def peers(self):
        peers = [self.device((self.first + d) % self.side, self.second) for d in range(1, self.side)]
        peers += [self.device(self.first, (self.second + d) % self.side) for d in range(1, self.side)]
        return [*peers, self.partner()]

    def greet(self):
        for peer in self.peers():
            pl.semaphore_signal(pltpu.get_barrier_semaphore(), inc=1, device_id=peer, device_id_type=MESH)

    def meet(self):
        pl.semaphore_wait(pltpu.get_barrier_semaphore(), 2 * self.side - 1)


def far_first(side):
    return sorted(range(1, side), key=lambda d: -min(d, side - d))


def remote(src, dst, send_sem, recv_sem, device):
    return pltpu.make_async_remote_copy(src_ref=src, dst_ref=dst, send_sem=send_sem, recv_sem=recv_sem, device_id=device, device_id_type=MESH)


def norm_rows(r_ref, gain, shift, buf, tile):
    rows = pl.ds(pl.multiple_of(tile * TILE, TILE), TILE)
    v = r_ref[rows, :].astype(F32)
    mean = jnp.mean(v, axis=-1, keepdims=True)
    v = v - mean
    var = jnp.mean(v * v, axis=-1, keepdims=True)
    buf[0, rows, :] = (v * lax.rsqrt(var + LN_EPS) * gain + shift).astype(BF16)


class Gather:
    def __init__(self, place, buf, send, recv):
        self.place, self.buf, self.send, self.recv = place, buf, send, recv
        self.half = buf.shape[1] // 2
        self.subs = self.half // TILE
        n = place.chips
        self.next = [place.device(*place.at_pos((place.pos + d) % n))["tp"] for d in (1, n - 1)]

    def hop(self, dr, s, k):
        rows = pl.ds(pl.multiple_of(dr * self.half + k * TILE, TILE), TILE)
        return remote(self.buf.at[s, rows], self.buf.at[s + 1, rows], self.send.at[dr, s, k], self.recv.at[dr, s, k],
                      {"tp": self.next[0] * (1 - dr) + self.next[1] * dr})

    def start(self, norm, before, meanwhile):
        norm(0)
        norm(self.subs)
        self.place.meet()
        before()

        def step(k, carry):
            norm(k)
            norm(self.subs + k)
            for dr in range(2):
                self.hop(dr, 0, k - 1).start()
            return carry
        lax.fori_loop(1, self.subs, step, 0)
        meanwhile()
        for dr in range(2):
            self.hop(dr, 0, self.subs - 1).start()

    def take(self, s, k):
        for dr in range(2):
            self.hop(dr, s - 1, k).wait_recv()

            @pl.when(s < self.place.chips - 1)
            def _():
                self.hop(dr, s, k).start()

    def sent(self, s):
        @pl.when(s < self.place.chips - 1)
        def _():
            for dr in range(2):
                for k in range(self.subs):
                    self.hop(dr, s, k).wait_send()

    def run(self, part):
        n = self.place.chips // 2
        for k in range(self.subs):
            self.take(1, k)

        def step(j, carry):
            for h in range(2):
                for k in range(self.subs):
                    @pl.when(j < n)
                    def _():
                        self.take(2 * j + h, k)
                    part(j - 1, h * self.subs + k)
            return carry
        lax.fori_loop(1, n + 1, step, 0)


class Scatter:
    def __init__(self, place, buf, r1, sums, mid, r2, s1_send, s1_recv, mid_send, mid_recv, s2_send, s2_recv):
        self.place, self.buf, self.r1, self.sums, self.mid, self.r2 = place, buf, r1, sums, mid, r2
        self.mid_send, self.mid_recv = mid_send, mid_recv
        self.s1_send, self.s1_recv, self.s2_send, self.s2_recv = s1_send, s1_recv, s2_send, s2_recv
        self.half = buf.shape[1] // 2

    def rows(self, dr):
        return pl.ds(dr * self.half, self.half)

    def first_copy(self, slot, dr, j, first, second):
        p = self.place
        return remote(self.buf.at[slot, self.rows(dr)], self.r1.at[j, second, self.rows(dr)], self.s1_send.at[j, second, dr],
                      self.s1_recv.at[j, second, dr], p.device(first, p.second))

    def send_rows(self, d, dr, begin, end):
        p = self.place
        second = (p.second + d) % p.side
        for away in far_first(p.side):
            first = (p.first + away) % p.side
            slot = self.slot_of(first, second, dr)

            @pl.when((slot >= begin) & (slot < end))
            def _():
                self.first_copy(slot, dr, p.side - 1 - away, first, second).start()

    def slot_of(self, first, second, dr):
        p = self.place
        pos = p.pos_of(first, second)
        return (p.pos + p.chips - pos) % p.chips if dr == 0 else (pos + p.chips - p.pos) % p.chips

    def arrived(self, second, dr):
        for j in range(self.place.side - 1):
            self.first_copy(0, dr, j, self.place.first, second).wait_recv()

    def total(self, second, dr, rows):
        v = self.buf[self.slot_of(self.place.first, second, dr), rows, :].astype(F32)
        for j in range(self.place.side - 1):
            v = v + self.r1[j, second, rows, :].astype(F32)
        return v

    def tile(self, dr, k):
        return pl.ds(pl.multiple_of(dr * self.half + k * TILE, TILE), TILE)

    def mid_copy(self, dr, k):
        p = self.place
        step = 1 if dr == 0 else p.side - 1
        rows = self.tile(dr, k)
        return remote(self.sums.at[1, rows], self.mid.at[rows], self.mid_send.at[dr, k], self.mid_recv.at[dr, k],
                      p.device(p.first, (p.second + step) % p.side))

    def end_copy(self, d, dr, k):
        p = self.place
        at = 0 if d == 1 else 1
        rows = self.tile(dr, k)
        return remote(self.sums.at[d - 1, rows], self.r2.at[at, rows], self.s2_send.at[at, dr, k], self.s2_recv.at[at, dr, k],
                      p.device(p.first, (p.second + d) % p.side))

    def add(self, d, dr, k, with_mid):
        second = (self.place.second + d) % self.place.side
        rows = self.tile(dr, k)
        v = self.total(second, dr, rows)
        if with_mid:
            self.mid_copy(dr, k).wait_recv()
            v = v + self.mid[rows, :]
        self.sums[d - 1, rows, :] = v

    def tiles(self, fn):
        def one(k, carry):
            fn(k)
            return carry
        lax.fori_loop(0, self.half // TILE, one, 0)

    def finish(self, res, bias, out_ref, meanwhile):
        p = self.place

        def pieces(group, with_mid, copy):
            for d, dr in group:
                self.arrived((p.second + d) % p.side, dr)

            def one(k):
                for d, dr in group:
                    self.add(d, dr, k, with_mid)
                    copy(d, dr, k).start()
            self.tiles(one)

        ends = [(1, 1), (p.side - 1, 0)] if p.side > 2 else [(1, 0), (1, 1)]
        pieces(ends, False, self.end_copy)
        if p.side > 2:
            pieces([(2, 0), (2, 1)], False, lambda d, dr, k: self.mid_copy(dr, k))
            more = [(1, 0), (p.side - 1, 1)]
            pieces(more, True, self.end_copy)
            ends = ends + more
        meanwhile()
        for dr in range(2):
            self.arrived(p.second, dr)

        def last(k):
            for dr in range(2):
                rows = self.tile(dr, k)
                for d, half in ends:
                    if half == dr:
                        self.end_copy(d, dr, k).wait_recv()
                v = self.total(p.second, dr, rows)
                for j in range(self.r2.shape[0]):
                    v = v + self.r2[j, rows, :]
                v = res[rows, :] + v + bias
                res[rows, :] = v
                out_ref[rows, :] = v.astype(out_ref.dtype)
        self.tiles(last)

        def sent(k):
            if p.side > 2:
                for dr in range(2):
                    self.mid_copy(dr, k).wait_send()
            for d, dr in ends:
                self.end_copy(d, dr, k).wait_send()
        self.tiles(sent)
        for dr in range(2):
            for j in range(p.side - 1):
                for second in range(p.side):
                    self.first_copy(0, dr, j, p.first, second).wait_send()


class Share:
    def __init__(self, place, pairs, local, send, recv):
        self.place, self.pairs, self.local, self.send, self.recv = place, pairs, local, send, recv

    def load(self, i):
        src, own, _ = self.pairs[i]
        return pltpu.make_async_copy(src, own, self.local.at[i])

    def give(self, i):
        _, own, other = self.pairs[i]
        return remote(own, other, self.send.at[i], self.recv.at[i], self.place.partner())


def layers_kernel(group_size, n_seq, r_ref, norm_ref, bout_ref, bdown_ref, bup_ref, wqkv_ref, wout_ref, wup_ref, wdown_ref, out_ref,
                 buf, wu, wd, bu, u, r1, sums, mid, r2, qkv, kvp, wo, w4, res,
                 wl, ws, wr, free, ag_send, ag_recv, ag2_send, ag2_recv, kv_send, kv_recv, a_send, a_recv, f_send, f_recv, w4_send, w4_recv,
                 p_send, p_recv, s_send, s_recv, s1_send, s1_recv, mid_send, mid_recv, s2_send, s2_recv):
    place = Place(group_size)
    slots, block, model = buf.shape
    side, hd, ff = place.side, w4.shape[1] // 2, wup_ref.shape[2]
    n_chunks, per_seq, width = block // TILE, block // n_seq, model // place.side
    per_row = side
    every = slots * TILE

    def widen(i, carry):
        rows = pl.ds(pl.multiple_of(i * TILE, TILE), TILE)
        res[rows, :] = r_ref[rows, :].astype(F32)
        return carry
    lax.fori_loop(0, n_chunks, widen, 0)

    def one_layer(layer, carry):
        share = Share(place, [(wout_ref.at[layer], wo.at[pl.ds(0, hd)], wo.at[pl.ds(hd, hd)])]
                      + [(wqkv_ref.at[layer, t], wu.at[:, pl.ds(t * hd, hd)], wu.at[:, pl.ds((3 + t) * hd, hd)]) for t in range(3)]
                      + [(bup_ref, bu.at[:, pl.ds(0, ff)], bu.at[:, pl.ds(ff, ff)]),
                         (wup_ref.at[layer], wu.at[:, pl.ds(0, ff)], wu.at[:, pl.ds(ff, ff)]),
                         (wdown_ref.at[layer], wd.at[pl.ds(0, ff)], wd.at[pl.ds(ff, ff)])], wl, ws, wr)
        area = [2 * hd + i * every for i in range(3)]

        def piece(i, n):
            return wd.at[pl.ds(area[i], every), pl.ds(pl.multiple_of(n * 2 * hd, 2 * hd), 2 * hd)]

        def heads(j, chunk):
            return (piece(2, chunk), piece(2, n_chunks + chunk), piece(1, n_chunks + chunk), piece(1, chunk))[j]

        def partial(chunk):
            over = chunk // per_row
            row = pl.multiple_of(area[0] + every * over * (chunk - per_row + 1), TILE)
            col = pl.multiple_of(width * (chunk * (1 - over) + (per_row - 1) * over), width)
            return row, pl.ds(col, width)

        def cell(chunk):
            return chunk // per_row, pl.ds(pl.multiple_of(chunk % per_row * width, width), width)

        place.greet()
        for i in range(1, 4):
            share.load(i).start()

        @pl.when(layer == 0)
        def _():
            share.load(0).start()
        gather = Gather(place, buf, ag_send, ag_recv)

        def norm(tile):
            norm_rows(res, norm_ref[layer, 0:1, :], norm_ref[layer, 1:2, :], buf, tile)

        def col(first):
            return pl.ds(pl.multiple_of(first * width, width), width)

        def w_copy(d, h):
            first = (place.first + d) % side
            rows = pl.ds(h * hd, hd)
            return remote(wo.at[rows, col(first)], w4.at[side - 1 - d, rows], w4_send.at[side - 1 - d, h], w4_recv.at[side - 1 - d, h],
                          place.device(first, place.second))

        def share_own(which):
            which.load(0).wait()
            which.give(0).start()

        def share_out(which):
            for d in far_first(side):
                w_copy(d, 0).start()

        def share_rest(which):
            which.give(0).wait_recv()
            for d in far_first(side):
                w_copy(d, 1).start()

        def share_qkv():
            for i in range(1, 4):
                share.load(i).wait()
                share.give(i).start()
        gather.start(norm, lambda: pl.when(layer == 0)(lambda: (share_own(share), share_out(share))[1]), share_qkv)
        pl.when(layer == 0)(lambda: share_rest(share))

        def kv_copy(j, h):
            pair = pl.ds(2 * j, 2)
            return remote(qkv.at[pair, :, pl.ds(3 * hd * h + hd, 2 * hd)], kvp.at[pair, :, pl.ds(2 * hd * (1 - h), 2 * hd)],
                          kv_send.at[j, h], kv_recv.at[j, h], place.partner())

        def qkv_part(j, i):
            if i % 2 == 0:
                if i == 0:
                    @pl.when(j == 0)
                    def _():
                        for t in range(3):
                            share.give(1 + t).wait_recv()
                cols = pl.ds(i // 2 * 2 * hd, 2 * hd)
                rows = buf[pl.ds(2 * j, 2)].reshape(2 * block, model)
                qkv[pl.ds(2 * j, 2), :, cols] = jnp.dot(rows, wu[:, cols], preferred_element_type=F32).astype(BF16).reshape(2, block, 2 * hd)
            if i == 5:
                for h in range(2):
                    kv_copy(j, h).start()
                gather.sent(2 * j)
                gather.sent(2 * j + 1)
        gather.run(qkv_part)
        for j in range(slots // 2):
            for h in range(2):
                kv_copy(j, h).wait_recv()
        for i in range(1, 4):
            share.give(i).wait_send()
        for i in (4, 5):
            share.load(i).start()

        nk = slots * per_seq

        def rows_of(chunk):
            return pl.ds(pl.multiple_of(chunk * TILE, TILE), TILE)

        def attend(chunk):
            seq = chunk * TILE // per_seq
            lower = chunk * TILE // (block // 2)
            keys = pl.ds(pl.multiple_of(seq * per_seq, per_seq), per_seq)

            def head_of(h, carry):
                def cols(base, k):
                    return pl.ds(pl.multiple_of(h * base + k * hd, hd), hd)
                q = qkv[:, rows_of(chunk), cols(3 * hd, 0)].reshape(every, hd)
                k0 = qkv[:, keys, cols(3 * hd, 1)].reshape(nk, hd)
                v0 = qkv[:, keys, cols(3 * hd, 2)].reshape(nk, hd)
                k1 = kvp[:, keys, cols(2 * hd, 0)].reshape(nk, hd)
                v1 = kvp[:, keys, cols(2 * hd, 1)].reshape(nk, hd)
                dims = (((1,), (1,)), ((), ()))
                s0 = lax.dot_general(q, k0, dims, preferred_element_type=F32) * hd ** -0.5
                s1 = lax.dot_general(q, k1, dims, preferred_element_type=F32) * hd ** -0.5
                top = jnp.maximum(jnp.max(s0, axis=-1, keepdims=True), jnp.max(s1, axis=-1, keepdims=True))
                e0 = jnp.exp(s0 - top)
                e1 = jnp.exp(s1 - top)
                inv = 1.0 / (jnp.sum(e0, axis=-1, keepdims=True) + jnp.sum(e1, axis=-1, keepdims=True))
                a = jnp.dot((e0 * inv).astype(BF16), v0, preferred_element_type=F32)
                a = (a + jnp.dot((e1 * inv).astype(BF16), v1, preferred_element_type=F32)).astype(BF16)
                for slot in range(slots):
                    pos = (place.pos + (slots - slot) * (1 - lower) + slot * lower) % slots
                    wd[pl.ds(pl.multiple_of(area[1] + pos * TILE, TILE), TILE),
                       pl.ds(pl.multiple_of(chunk * 2 * hd + h * hd, hd), hd)] = a[slot * TILE:(slot + 1) * TILE]
                return carry
            lax.fori_loop(0, 2, head_of, 0)
            for d in near:
                a_copy(chunk, d).start()

        near = (1, side - 1)

        def a_copy(chunk, d):
            return remote(heads(side - 1, chunk), heads(side - 1 - d, chunk), a_send.at[chunk, d // 2], a_recv.at[chunk, d // 2],
                          place.device((place.first + d) % side, place.second))

        def f_copy(chunk, h):
            cols = pl.ds(h * hd, hd)
            return remote(heads(2 - 2 * h, chunk).at[:, cols], heads(1, chunk).at[:, cols], f_send.at[chunk, h], f_recv.at[chunk, h],
                          place.device((place.first + (1 if h == 0 else side - 1)) % side, place.second))

        def forward(chunk):
            for d in near:
                a_copy(chunk, d).wait_recv()
            for h in range(2):
                f_copy(chunk, h).start()

            @pl.when(chunk == 0)
            def _():
                for i in (4, 5):
                    share.load(i).wait()
                    share.give(i).start()

        def p_copy(chunk, d):
            second = (place.second + d) % side
            row, cols = partial(chunk)
            at, there = cell(chunk)
            return remote(wd.at[pl.ds(pl.multiple_of(row + second * side * TILE, TILE), side * TILE), cols],
                          r1.at[side - 1 - d, at, pl.ds(0, side * TILE), there], p_send.at[chunk, side - 1 - d], p_recv.at[chunk, side - 1 - d],
                          place.device(place.first, second))

        def project(chunk):
            @pl.when(chunk == 0)
            def _():
                for d in range(1, side):
                    for h in range(2):
                        w_copy(d, h).wait_recv()
            for h in range(2):
                f_copy(chunk, h).wait_recv()
            half = width // 2
            row, cols = partial(chunk)
            for c in range(2):
                own = pl.ds(pl.multiple_of(place.first * width + c * half, half), half)
                v = jnp.dot(heads(side - 1, chunk)[...], wo[:, own], preferred_element_type=F32)
                for j in range(side - 1):
                    v = v + jnp.dot(heads(j, chunk)[...], w4[j, :, pl.ds(c * half, half)], preferred_element_type=F32)
                wd[pl.ds(row, every), pl.ds(pl.multiple_of(cols.start + c * half, half), half)] = v.astype(BF16)
            for d in far_first(side):
                p_copy(chunk, d).start()

        def s_copy(chunk, d):
            first = (place.first + d) % side
            at, there = cell(chunk)
            i = (first + place.second) % side
            return remote(sums.at[at, pl.ds(pl.multiple_of(i * TILE, TILE), TILE), there],
                          r2.at[0, rows_of(chunk), pl.ds((side - 1 - d) * width, width)], s_send.at[chunk, side - 1 - d], s_recv.at[chunk, side - 1 - d],
                          place.device(first, place.second))

        def add(chunk):
            for d in range(1, side):
                p_copy(chunk, d).wait_recv()
            row, cols = partial(chunk)
            at, there = cell(chunk)

            def one(i, carry):
                rows = rows_of(i)
                v = wd[pl.ds(pl.multiple_of(row + (place.second * side + i) * TILE, TILE), TILE), cols].astype(F32)
                for j in range(side - 1):
                    v = v + r1[j, at, rows, there].astype(F32)
                sums[at, rows, there] = v
                return carry
            lax.fori_loop(0, side, one, 0)
            for d in far_first(side):
                s_copy(chunk, d).start()

        gather2 = Gather(place, buf, ag2_send, ag2_recv)
        subs = gather2.subs

        def output(chunk):
            rows = rows_of(chunk)
            at, there = cell(chunk)

            def put(first, v):
                res[rows, col(first)] = res[rows, col(first)] + v + bout_ref[pl.ds(layer, 1), col(first)]
            put(place.first, sums[at, pl.ds(pl.multiple_of((place.first + place.second) % side * TILE, TILE), TILE), there])
            for j in range(side - 1):
                s_copy(chunk, side - 1 - j).wait_recv()
                put((place.first + 1 + j) % side, r2[0, rows, pl.ds(j * width, width)])
            norm_rows(res, norm_ref[layer, 2:3, :], norm_ref[layer, 3:4, :], buf, chunk)

            @pl.when(chunk > 0)
            def _():
                gather2.hop((chunk - 1) // subs, 0, (chunk - 1) % subs).start()

        lag = n_chunks // 2
        stages = ((attend, 0), (forward, lag - 1), (project, lag), (add, lag + 1), (output, lag + 2))

        def step(i, carry):
            for stage, at in stages:
                @pl.when((i >= at) & (i < at + n_chunks))
                def _():
                    stage(i - at)
            return carry
        lax.fori_loop(0, n_chunks + lag + 2, step, 0)

        def done(chunk, carry):
            for d in range(1, side):
                p_copy(chunk, d).wait_send()
                s_copy(chunk, d).wait_send()
            for d in near:
                a_copy(chunk, d).wait_send()
            for h in range(2):
                f_copy(chunk, h).wait_send()
            return carry
        lax.fori_loop(0, n_chunks, done, 0)
        gather2.hop(1, 0, subs - 1).start()
        for d in range(1, side):
            for h in range(2):
                w_copy(d, h).wait_send()
        share.give(0).wait_send()
        share.load(6).start()
        pl.semaphore_signal(free, inc=1, device_id=place.partner(), device_id_type=MESH)
        for j in range(slots // 2):
            for h in range(2):
                kv_copy(j, h).wait_send()

        scatter = Scatter(place, buf, r1, sums, mid, r2, s1_send, s1_recv, mid_send, mid_recv, s2_send, s2_recv)
        up_w, down_w = ff // 2, model // 4

        def up(j, c):
            rows = buf[pl.ds(2 * j, 2)].reshape(2 * block, model)
            cols = pl.ds(c * up_w, up_w)
            hidden = jnp.dot(rows, wu[:, cols], preferred_element_type=F32) + bu[pl.ds(layer, 1), cols]
            u[:, cols] = jax.nn.gelu(hidden, approximate=True).astype(BF16)

        def down(j, c):
            cols = pl.ds(c * down_w, down_w)
            buf[pl.ds(2 * j, 2), :, cols] = jnp.dot(u[...], wd[:, cols], preferred_element_type=F32).astype(BF16).reshape(2, block, down_w)

        def mlp_part(j, i):
            if i == 0:
                @pl.when(j == 0)
                def _():
                    share.load(6).wait()
                    pl.semaphore_wait(free, 1)
                    share.give(6).start()
                    share.give(4).wait_recv()
                    share.give(5).wait_recv()

                @pl.when(j == slots // 2 - 1)
                def _():
                    for d, dr in ((2, 0), (2, 1), (1, 0), (3, 1)):
                        scatter.send_rows(d, dr, 0, slots - 2)

                @pl.when(j == slots // 2 - 3)
                def _():
                    for d, dr in ((1, 1), (3, 0)):
                        scatter.send_rows(d, dr, 0, slots // 2)
                up(j, 0)
                up(j, 1)
            elif i == 1:
                up(j, 2)
            elif i == 2:
                up(j, 3)
            elif i == 3:
                @pl.when(j == 0)
                def _():
                    share.give(6).wait_recv()
                gather2.sent(2 * j)
                gather2.sent(2 * j + 1)
                down(j, 0)
            elif i == 4:
                down(j, 1)
            else:
                down(j, 2)
                down(j, 3)
        gather2.run(mlp_part)
        for d, dr in ((1, 0), (3, 1)):
            scatter.send_rows(d, dr, slots - 2, slots)
        for dr in range(2):
            scatter.send_rows(0, dr, 0, slots)
        following = Share(place, [(wout_ref.at[layer + 1], wo.at[pl.ds(0, hd)], wo.at[pl.ds(hd, hd)])], wl, ws, wr)
        more = pl.when(layer + 1 < wqkv_ref.shape[0])
        more(lambda: following.load(0).start())
        more(lambda: share_own(following))
        scatter.finish(res, bdown_ref[pl.ds(layer, 1), :], out_ref, lambda: more(lambda: (share_out(following), share_rest(following))[1]))
        for i in (4, 5, 6):
            share.give(i).wait_send()
        return carry
    lax.fori_loop(0, wqkv_ref.shape[0], one_layer, 0)


def solution(mesh):
    group_size = mesh.shape["tp"]
    side = math.isqrt(group_size // 2)
    chips = side * side
    dma = pltpu.SemaphoreType.DMA
    vmem = pl.BlockSpec(memory_space=pltpu.VMEM)
    hbm = pl.BlockSpec(memory_space=pl.ANY)

    def local_layers(hidden_in, norms, w_qkv, w_out, b_out, w_up, b_up, w_down, b_down):
        n_seq, per_seq, model = hidden_in.shape
        n_layers, head_dim, ff = w_qkv.shape[0], w_qkv.shape[-1], w_up.shape[-1]
        block = n_seq * per_seq
        subs = block // 2 // TILE
        n_chunks = block // TILE
        residual = hidden_in.reshape(block, model)
        w_qkv = w_qkv.transpose(0, 2, 3, 1, 4).reshape(n_layers, 3, model, head_dim)
        w_out = w_out.reshape(n_layers, head_dim, model)
        residual = pl.pallas_call(
            functools.partial(layers_kernel, group_size, n_seq), name="layers",
            out_shape=jax.ShapeDtypeStruct((block, model), BF16),
            in_specs=[vmem] * 4 + [hbm] * 5, out_specs=vmem,
            scratch_shapes=[
                pltpu.VMEM((chips, block, model), BF16), pltpu.VMEM((model, 2 * ff), BF16), pltpu.VMEM((2 * ff, model), BF16),
                pltpu.VMEM((n_layers, 2 * ff), F32), pltpu.VMEM((2 * block, 2 * ff), BF16), pltpu.VMEM((side - 1, side, block, model), BF16),
                pltpu.VMEM((side - 1, block, model), F32), pltpu.VMEM((block, model), F32), pltpu.VMEM((2, block, model), F32),
                pltpu.VMEM((chips, block, 6 * head_dim), BF16), pltpu.VMEM((chips, block, 4 * head_dim), BF16),
                pltpu.VMEM((2 * head_dim, model), BF16), pltpu.VMEM((side - 1, 2 * head_dim, model // side), BF16),
                pltpu.VMEM((block, model), F32),
                *[dma((7,))] * 3, pltpu.SemaphoreType.REGULAR, *[dma((2, chips - 1, subs))] * 4, *[dma((chips // 2, 2))] * 2,
                *[dma((n_chunks, 2))] * 4, *[dma((side - 1, 2))] * 2, *[dma((n_chunks, side - 1))] * 4,
                *[dma((side - 1, side, 2))] * 2, *[dma((2, subs))] * 2, *[dma((2, 2, subs))] * 2],
            compiler_params=pltpu.CompilerParams(collective_id=0, has_side_effects=True, vmem_limit_bytes=VMEM_LIMIT),
        )(residual, norms, b_out, b_down, b_up, w_qkv, w_out, w_up, w_down)
        return residual.reshape(n_seq, per_seq, model)

    in_specs = (P('dp', 'tp', None), P(), P(None, None, None, 'tp', None), P(None, 'tp', None, None), P(), P(None, None, 'tp'), P(None, 'tp'), P(None, 'tp', None), P())
    return jax.shard_map(local_layers, mesh=mesh, in_specs=in_specs, out_specs=P('dp', 'tp', None), check_vma=False)
```
